256 devices in a mesh: seq: 16 (over z, core), head: 4 (over x), batch: 4 (over y).
Axes of the slice: x: 4, y: 4, z: 8, core: 2. Of those that a mesh axis runs over, the one named last changes fastest.
Arguments:
- queries: bfloat16 [4, 8192, 8, 8, 128], P('batch', 'seq', 'head'), may hold values from -160 to 160
- key_rows: bfloat16 [4, 8192, 8, 128], P('batch', 'seq'), may hold values from -6 to 6
- value_rows: bfloat16 [4, 8192, 8, 128], P('batch', 'seq'), may hold values from -6 to 6
- compressed: bfloat16 [4, 128, 8, 128], P('batch', 'seq'), may hold values from -6 to 6
- chosen: int32 [4, 128, 8, 16], P('batch', 'seq'), may hold values from 0 to 127, as said below
Outputs:
- block_scores: float32 [4, 128, 8, 128], P('batch', 'seq', 'head')
- attended: bfloat16 [4, 8192, 8, 8, 128], P('batch', 'seq', 'head')
The draws below stay inside these ranges and needn't reach their ends.
Inputs may be any that keep to these rules, and one draw needn't show every extreme that they name: `chosen`: every entry is at most its own tile number, and entry 0 of every row is the tile's own block. Over the tiles of one device of seq and one group, at most 2 different blocks of any other device are named, and every device after the first names exactly 2 blocks of the first device for each group.
All inputs are finite; a program needn't handle non-finite values.
Results may differ from the reference program's by a relative error of at most 0.008.
Values may be sent and summed in bfloat16 or wider, within the bound.
No kernel may reach another device: no remote copies, remote signals or barrier semaphores. Data moves between devices by JAX's collectives and lax.ppermute only.
A program may use at most 128 MiB of HBM per device.

```python
import jax
import jax.numpy as jnp
from jax import lax

HPG = 8
G = 8
DH = 128
BLOCK = 64
TOPN = 16
BATCH = 4
SEQ_LEN = 8192
BLK_DEV = 8
NBLK = 128


def fields(key):
    key_one, key_two, key_three = jax.random.split(jax.random.fold_in(key, 71), 3)
    key_base = jnp.clip(jax.random.normal(key_one, (BATCH, SEQ_LEN, G, DH), jnp.float32), -5.0, 5.0)
    comp_base = jnp.clip(jax.random.normal(key_two, (BATCH, NBLK, G, DH), jnp.float32), -5.0, 5.0)
    query_base = jnp.clip(jax.random.normal(key_three, (BATCH, SEQ_LEN, HPG, G, DH), jnp.float32), -5.0, 5.0)
    return (query_base, key_base, comp_base)


def draw_queries(key, part):
    return fields(key)[0].astype(jnp.bfloat16)


def draw_key_rows(key, part):
    return fields(key)[1].astype(jnp.bfloat16)


def draw_compressed(key, part):
    return fields(key)[2].astype(jnp.bfloat16)


def draw_chosen(key, part):
    key_one, key_two, key_three = jax.random.split(jax.random.fold_in(key, 5), 3)
    shards = NBLK // BLK_DEV
    lower_pick = jax.random.randint(key_one, (BATCH, shards, G, shards), 0, BLK_DEV)
    upper_pick = (lower_pick + 1 + jax.random.randint(key_two, (BATCH, shards, G, shards), 0, BLK_DEV - 1)) % BLK_DEV
    offsets = jnp.arange(shards, dtype=jnp.int32) * BLK_DEV
    candidates = jnp.stack([lower_pick + offsets, upper_pick + offsets], axis=-1).reshape(BATCH, shards, G, shards * 2)
    tile_ids = jnp.arange(NBLK, dtype=jnp.int32)
    span_ids = tile_ids // BLK_DEV
    inner_ids = tile_ids % BLK_DEV
    remote_count = 2 * span_ids
    pool_size = remote_count + inner_ids + 1
    random_pointer = jax.random.randint(key_three, (BATCH, NBLK, G, TOPN), 0, pool_size[None, :, None, None])
    slot_ids = jnp.arange(TOPN, dtype=jnp.int32)[None, None, None, :]
    own_pointer = (remote_count + inner_ids)[None, :, None, None]
    sink_pointer = (inner_ids % 2)[None, :, None, None]
    has_remote = (span_ids > 0)[None, :, None, None]
    pointer = jnp.where(slot_ids == 0, own_pointer, jnp.where((slot_ids == 1) & has_remote, sink_pointer, random_pointer))
    tile_candidates = candidates[:, span_ids]
    remote_ids = jnp.take_along_axis(tile_candidates, jnp.clip(pointer, 0, shards * 2 - 1), axis=-1)
    local_ids = (span_ids * BLK_DEV - remote_count)[None, :, None, None] + pointer
    return jnp.where(pointer < remote_count[None, :, None, None], remote_ids, local_ids).astype(jnp.int32)


def levels(key, extent, pieces, least, top_value):
    gain = 1.0
    for position, parts in pieces:
        draws = jax.random.uniform(jax.random.fold_in(jax.random.fold_in(key, 6), position), (parts,), jnp.float32, least / len(pieces), top_value / len(pieces))
        gain = gain * jnp.repeat(jnp.exp(draws), extent[position] // parts).reshape((-1,) + (1,) * (len(extent) - 1 - position))
    return gain


def gaussian(key, shape, scale, most, pieces=(), kind=jnp.bfloat16):
    result = scale * jax.random.normal(key, shape, jnp.float32)
    if pieces:
        result = result * levels(key, shape, pieces, -0.22, 0.18)
    return jnp.clip(result, -most, most).astype(kind)


def setup_inputs(seed: int = 0) -> dict:
    key_of = jax.random.split(jax.random.key(seed), 6)
    return {
        "queries": draw_queries(jax.random.fold_in(key_of[5], 71), 0),
        "key_rows": draw_key_rows(jax.random.fold_in(key_of[5], 71), 0),
        "value_rows": gaussian(key_of[2], (BATCH, SEQ_LEN, G, DH), 1.0, 6.0, ((0, 4), (1, 16))),
        "compressed": draw_compressed(jax.random.fold_in(key_of[5], 71), 0),
        "chosen": draw_chosen(jax.random.fold_in(key_of[5], 71), 0),
    }


def softmax_parts(scores):
    row_top = jnp.max(scores, axis=-1, keepdims=True)
    weights = jnp.exp(scores - row_top)
    return weights, jnp.sum(weights, axis=-1, keepdims=True)


def one_sequence(inputs):
    query_seq, key_seq, value_seq, compressed_seq, chosen_seq = inputs
    score_scale = DH ** -0.5
    tile_step = 2
    rounds = NBLK // tile_step
    key_blocks = key_seq.reshape(NBLK, BLOCK, G, DH)
    value_blocks = value_seq.reshape(NBLK, BLOCK, G, DH)
    all_blocks = jnp.arange(NBLK, dtype=jnp.int32)
    group_ids = jnp.arange(G, dtype=jnp.int32)[None, :, None]
    comp_wide = compressed_seq.astype(jnp.float32)

    def per_round(round_in):
        query_part, pick_part, round_id = round_in
        query_pos = round_id * (tile_step * BLOCK) + jnp.arange(tile_step * BLOCK, dtype=jnp.int32)
        query_wide = query_part.astype(jnp.float32)
        logits = jnp.einsum("qhgd,ngd->qhgn", query_wide, comp_wide) * score_scale
        seen = all_blocks[None, :] <= (query_pos // BLOCK)[:, None]
        logits = jnp.where(seen[:, None, None, :], logits, -jnp.inf)
        weights, totals = softmax_parts(logits)
        probability = weights / totals
        pooled = jnp.sum(probability.reshape(tile_step, BLOCK, HPG, G, NBLK), axis=(1, 2))
        tile_ids = round_id * tile_step + jnp.arange(tile_step, dtype=jnp.int32)
        factor = (tile_ids + 1).astype(jnp.float32) / (BLOCK * HPG)
        scores_out = pooled * factor[:, None, None]
        key_sel = key_blocks[pick_part, :, group_ids, :].reshape(tile_step, G, TOPN * BLOCK, DH)
        value_sel = value_blocks[pick_part, :, group_ids, :].reshape(tile_step, G, TOPN * BLOCK, DH)
        key_pos = (pick_part[..., None] * BLOCK + jnp.arange(BLOCK, dtype=jnp.int32)).reshape(tile_step, G, TOPN * BLOCK)
        query_tiles = query_wide.reshape(tile_step, BLOCK, HPG, G, DH)
        scores = jnp.einsum("tqhgd,tgkd->tghqk", query_tiles, key_sel.astype(jnp.float32)) * score_scale
        tile_pos = query_pos.reshape(tile_step, BLOCK)
        visible = key_pos[:, :, None, None, :] <= tile_pos[:, None, None, :, None]
        scores = jnp.where(visible, scores, -jnp.inf)
        weights, totals = softmax_parts(scores)
        rounded = weights.astype(jnp.bfloat16)
        mixed = jnp.einsum("tghqk,tgkd->tqhgd", rounded.astype(jnp.float32), value_sel.astype(jnp.float32))
        attended = (mixed / jnp.transpose(totals, (0, 3, 2, 1, 4))).astype(jnp.bfloat16)
        return scores_out, attended.reshape(tile_step * BLOCK, HPG, G, DH)

    round_ids = jnp.arange(rounds, dtype=jnp.int32)
    scores_out, attended = lax.map(per_round, (query_seq.reshape(rounds, tile_step * BLOCK, HPG, G, DH), chosen_seq.reshape(rounds, tile_step, G, TOPN), round_ids))
    return scores_out.reshape(NBLK, G, NBLK), attended.reshape(SEQ_LEN, HPG, G, DH)


def reference(queries, key_rows, value_rows, compressed, chosen):
    block_scores, attended = lax.map(one_sequence, (queries, key_rows, value_rows, compressed, chosen))
    return block_scores, attended
```

```python
import functools
import math

import jax
import jax.numpy as jnp
from jax import lax
from jax.experimental import pallas as pl
from jax.experimental.pallas import tpu as pltpu
from jax.sharding import PartitionSpec as P


HPG = 8
GROUPS = 8
DH = 128
BLOCK = 64
TOPN = 16
NBLK = 128
SHARDS = 16
CHIPS = 8
COLS = 4
TOK = 512
TILES = 8
COMP_PAD = 16
PIECE = 2 * TOK + COMP_PAD
PARTS = 8
CHUNKS = 2
TOK_CHUNK = TOK // CHUNKS
TILES_CHUNK = TILES // CHUNKS
KEYS = TOPN * BLOCK
ROWS = HPG * BLOCK
COMP_ROWS = SHARDS * COMP_PAD
FAR = -1.0e9
EXP2_SCALE = DH**-0.5 * math.log2(math.e)
NT = (((1,), (1,)), ((), ()))
TN = (((0,), (0,)), ((), ()))


def iota(shape, dim):
    return lax.broadcasted_iota(jnp.int32, shape, dim)


def dot(lhs, rhs, dims=(((1,), (0,)), ((), ()))):
    return lax.dot_general(lhs, rhs, dims, preferred_element_type=jnp.float32)


def one_hot(cond):
    return jnp.where(cond, 1.0, 0.0).astype(jnp.bfloat16)


def split_pools(place, keys, values, comp, own, other):
    mine = place[0] * 2 + place[1]
    theirs = place[0] * 2 + 1 - place[1]
    step = 32
    row = iota((2 * step, step * GROUPS), 0)
    col = iota((2 * step, step * GROUPS), 1)
    group = jnp.where(row < step, mine, theirs)
    pick = one_hot(col == (row % step) * GROUPS + group)
    for i in range(TOK // step):
        rows = pl.ds(i * step * GROUPS, step * GROUPS)
        both = jnp.concatenate([keys[rows, :], values[rows, :]], axis=1)
        got = dot(pick, both).astype(jnp.bfloat16)
        own[pl.ds(i * step, step), :] = got[:step, :DH]
        own[pl.ds(TOK + i * step, step), :] = got[:step, DH:]
        other[pl.ds(i * step, step), :] = got[step:, :DH]
        other[pl.ds(TOK + i * step, step), :] = got[step:, DH:]
    row = iota((2 * COMP_PAD, TILES * GROUPS), 0)
    col = iota((2 * COMP_PAD, TILES * GROUPS), 1)
    group = jnp.where(row < COMP_PAD, mine, theirs)
    block = row % COMP_PAD
    got = dot(one_hot((col == block * GROUPS + group) & (block < TILES)), comp[...]).astype(jnp.bfloat16)
    own[pl.ds(2 * TOK, COMP_PAD), :] = got[:COMP_PAD]
    other[pl.ds(2 * TOK, COMP_PAD), :] = got[COMP_PAD:]


def row_of(r, place):
    part = r // 32
    head = (r // 16) % 2
    token = r % 16
    group = 2 * ((place[0] + part // 2) % COLS) + (place[1] + part % 2) % 2
    return token * 16 + head * GROUPS + group


def split_queries(tokens, place, queries, *parts):
    shape = (256, 256)
    pick = one_hot(iota(shape, 1) == row_of(iota(shape, 0), place))
    for i in range(tokens // 32):
        pair = jnp.concatenate([queries[pl.ds(i * 512, 256), :], queries[pl.ds(i * 512 + 256, 256), :]], axis=1)
        got = dot(pick, pair).astype(jnp.bfloat16)
        for k in range(PARTS):
            for j in range(2):
                rows = got[k * 32 + j * 16 : k * 32 + j * 16 + 16]
                parts[k][j, pl.ds(i * 32, 16), :] = rows[:, :DH]
                parts[k][j, pl.ds(i * 32 + 16, 16), :] = rows[:, DH:]


def join_outputs(tokens, place, *refs):
    parts, out = refs[:-1], refs[-1]
    shape = (256, 256)
    pick = one_hot(iota(shape, 0) == row_of(iota(shape, 1), place))
    for i in range(tokens // 32):
        halves = []
        for h in range(2):
            at = pl.ds(i * 32 + h * 16, 16)
            halves.append(jnp.concatenate([parts[k][j, at, :] for k in range(PARTS) for j in range(2)], axis=0))
        got = dot(pick, jnp.concatenate(halves, axis=1)).astype(jnp.bfloat16)
        out[pl.ds(i * 512, 256), :] = got[:, :DH]
        out[pl.ds(i * 512 + 256, 256), :] = got[:, DH:]


def attend(chunk, place, picks, *refs):
    pieces = refs[: 2 * CHIPS]
    queries = refs[2 * CHIPS : 2 * CHIPS + PARTS]
    outs = refs[2 * CHIPS + PARTS : 2 * CHIPS + 2 * PARTS]
    pooled = refs[2 * CHIPS + 2 * PARTS]
    pool, comp, mask, hot, scores, weights, sems = refs[2 * CHIPS + 2 * PARTS + 1 :]
    core, chip = place[1], place[2]
    copies = []
    for k in range(CHIPS):
        for h in range(2):
            slot = 2 * ((chip + k) % CHIPS) + (core + h) % 2
            copies.append(pltpu.make_async_copy(pieces[2 * k + h], pool.at[slot], sems.at[2 * k + h]))
    for copy in copies:
        copy.start()
    shape = (2 * BLOCK, DH)
    row = iota(shape, 0)
    hidden = (row >= BLOCK) & (row - BLOCK > iota(shape, 1))
    mask[...] = jnp.where(hidden, FAR, 0.0).astype(jnp.bfloat16)
    shape = (ROWS, DH)
    hot[...] = one_hot(iota(shape, 0) % BLOCK == iota(shape, 1))
    for copy in copies:
        copy.wait()
    for s in range(SHARDS):
        comp[pl.ds(s * COMP_PAD, COMP_PAD), :] = pool[s, pl.ds(2 * TOK, COMP_PAD), :]
    comp_row = iota((COMP_ROWS, ROWS), 0)
    comp_block = jnp.where(comp_row % COMP_PAD < TILES, comp_row // COMP_PAD * TILES + comp_row % COMP_PAD, NBLK)

    def one_tile(local, half):
        tile = chunk * TILES_CHUNK + local
        shard = 2 * chip + (core + half) % 2
        number = shard * TILES + tile
        at = pl.ds(pl.multiple_of(local * BLOCK, BLOCK), BLOCK)
        query = jnp.concatenate([queries[2 * dx + half][j, at, :] for dx in range(COLS) for j in range(2)], axis=0)
        wide = jnp.concatenate([query, hot[...]], axis=1)
        ids = [picks[(half * TILES + tile) * TOPN + b] for b in range(TOPN)]

        def block_of(n, offset):
            return pool[n // TILES, pl.ds(pl.multiple_of(offset + n % TILES * BLOCK, BLOCK), BLOCK), :]

        keys = []
        for n in ids:
            own = jnp.where(n == number, BLOCK, 0)
            keys.append(jnp.concatenate([block_of(n, 0), mask[pl.ds(pl.multiple_of(own, BLOCK), BLOCK), :]], axis=1))
        scores[half] = dot(jnp.concatenate(keys, axis=0), wide, NT)
        logits = jnp.where(comp_block <= number, dot(comp[...], query, NT), -jnp.inf)
        top = jnp.max(logits, axis=0, keepdims=True)
        raised = jnp.exp2((logits - top) * EXP2_SCALE)
        prob = raised * (1.0 / jnp.sum(raised, axis=0, keepdims=True))
        folded = prob[:, :128] + prob[:, 128:256] + prob[:, 256:384] + prob[:, 384:]
        pooled[half, pl.ds(local, 1), :] = jnp.sum(folded.T, axis=0, keepdims=True)
        top = jnp.max(scores[half], axis=0, keepdims=True)
        total = jnp.zeros((8, ROWS), jnp.float32)
        for b in range(TOPN):
            rows = pl.ds(b * BLOCK, BLOCK)
            weight = jnp.exp2((scores[half, rows, :] - top) * EXP2_SCALE)
            total = total + jnp.sum(weight.reshape(BLOCK // 8, 8, ROWS), axis=0)
            weights[half, rows, :] = weight.astype(jnp.bfloat16)
        total = jnp.sum(total, axis=0, keepdims=True)
        values = jnp.concatenate([block_of(n, TOK) for n in ids], axis=0)
        mixed = dot(values, weights[half], TN) / total
        result = mixed.T.astype(jnp.bfloat16)
        for dx in range(COLS):
            for j in range(2):
                r = (dx * 2 + j) * BLOCK
                outs[2 * dx + half][j, at, :] = result[r : r + BLOCK]

    def step(local, carry):
        one_tile(local, 0)
        one_tile(local, 1)
        return carry

    lax.fori_loop(0, TILES_CHUNK, step, 0)


SMEM = pl.BlockSpec(memory_space=pltpu.SMEM)
VMEM = pl.BlockSpec(memory_space=pltpu.VMEM)
ANY = pl.BlockSpec(memory_space=pl.ANY)


def bf16(*shape):
    return jax.ShapeDtypeStruct(shape, jnp.bfloat16)


def call_split_pools(place, keys, values, comp):
    return pl.pallas_call(
        split_pools,
        in_specs=[SMEM, VMEM, VMEM, VMEM],
        out_specs=[VMEM, VMEM],
        out_shape=[bf16(PIECE, DH)] * 2,
        name="split_pools",
    )(place, keys, values, comp)


def call_split_queries(place, queries):
    steps = 4
    tokens = TOK // steps
    return pl.pallas_call(
        functools.partial(split_queries, tokens),
        grid=(steps,),
        in_specs=[SMEM, pl.BlockSpec((tokens * 16, DH), lambda i: (i, 0))],
        out_specs=[pl.BlockSpec((2, tokens, DH), lambda i: (0, i, 0))] * PARTS,
        out_shape=[bf16(2, TOK, DH)] * PARTS,
        name="split_queries",
    )(place, queries)


def call_attend(chunk, place, picks, pieces, queries):
    return pl.pallas_call(
        functools.partial(attend, chunk),
        grid=(1,),
        in_specs=[SMEM, SMEM]
        + [ANY] * (2 * CHIPS)
        + [pl.BlockSpec((2, TOK_CHUNK, DH), lambda i: (0, chunk, 0))] * PARTS,
        out_specs=[pl.BlockSpec((2, TOK_CHUNK, DH), lambda i: (0, 0, 0))] * PARTS
        + [pl.BlockSpec((2, TILES_CHUNK, COMP_ROWS), lambda i: (0, 0, 0))],
        out_shape=[bf16(2, TOK_CHUNK, DH)] * PARTS
        + [jax.ShapeDtypeStruct((2, TILES_CHUNK, COMP_ROWS), jnp.float32)],
        scratch_shapes=[
            pltpu.VMEM((SHARDS, PIECE, DH), jnp.bfloat16),
            pltpu.VMEM((COMP_ROWS, DH), jnp.bfloat16),
            pltpu.VMEM((2 * BLOCK, DH), jnp.bfloat16),
            pltpu.VMEM((ROWS, DH), jnp.bfloat16),
            pltpu.VMEM((2, KEYS, ROWS), jnp.float32),
            pltpu.VMEM((2, KEYS, ROWS), jnp.bfloat16),
            pltpu.SemaphoreType.DMA((2 * CHIPS,)),
        ],
        name="attend",
    )(place, picks, *pieces, *queries)


def call_join_outputs(place, parts):
    steps = CHUNKS
    return pl.pallas_call(
        functools.partial(join_chunk),
        grid=(steps,),
        in_specs=[SMEM] + [pl.BlockSpec((2, TOK_CHUNK, DH), lambda i: (0, 0, 0))] * (PARTS * CHUNKS),
        out_specs=pl.BlockSpec((TOK_CHUNK * 16, DH), lambda i: (i, 0)),
        out_shape=bf16(TOK * 16, DH),
        name="join_outputs",
    )(place, *parts)


def join_chunk(place, *refs):
    parts, out = refs[:-1], refs[-1]
    for chunk in range(CHUNKS):

        @pl.when(pl.program_id(0) == chunk)
        def _():
            join_outputs(TOK_CHUNK, place, *parts[chunk * PARTS : (chunk + 1) * PARTS], out)


def by_seq(value, move):
    return lax.ppermute(value, "seq", [(s, move(s // 2, s % 2)) for s in range(SHARDS)])


def to_seq(chip, core):
    return chip % CHIPS * 2 + core % 2


def by_part(value, dx, dc, back):
    if dx == 0 and dc == 0:
        return value
    pairs = []
    for s in range(SHARDS):
        for x in range(COLS):
            there = (s ^ dc) * COLS + (x + dx) % COLS
            here = s * COLS + x
            pairs.append((there, here) if back else (here, there))
    return lax.ppermute(value, ("seq", "head"), pairs)


def local(queries, key_rows, value_rows, compressed, chosen):
    seq = lax.axis_index("seq")
    col = lax.axis_index("head")
    chip, core = seq // 2, seq % 2
    place = jnp.stack([col, core, chip]).astype(jnp.int32)
    own, other = call_split_pools(
        place, key_rows.reshape(TOK * GROUPS, DH), value_rows.reshape(TOK * GROUPS, DH), compressed.reshape(TILES * GROUPS, DH)
    )
    pieces = [None] * (2 * CHIPS)
    pieces[0] = own
    pieces[1] = by_seq(other, lambda z, c: to_seq(z, c + 1))
    up, down = [own, other], [own, other]
    for k in range(1, 4):
        for h in range(2):
            turn = h if k == 1 else 0
            up[h] = by_seq(up[h], lambda z, c: to_seq(z + 1, c + turn))
            down[h] = by_seq(down[h], lambda z, c: to_seq(z - 1, c + turn))
            pieces[2 * (CHIPS - k) + h] = up[h]
            pieces[2 * k + h] = down[h]
    for h in range(2):
        onward = jnp.where(core == 0, up[h], down[h])
        pieces[2 * 4 + h] = by_seq(onward, lambda z, c: to_seq(z + (1 if c == 0 else -1), c))
    parts = call_split_queries(place, queries.reshape(TOK * 16, DH))
    moved = [by_part(parts[k], k // 2, k % 2, False) for k in range(PARTS)]
    groups = chosen[0].transpose(1, 0, 2)
    mine = lax.dynamic_index_in_dim(groups, 2 * col + core, 0, False)
    theirs = lax.dynamic_index_in_dim(groups, 2 * col + 1 - core, 0, False)
    theirs = by_seq(theirs, lambda z, c: to_seq(z, c + 1))
    picks = jnp.concatenate([mine, theirs]).reshape(-1)
    joined, pooled = [], []
    for chunk in range(CHUNKS):
        *outs, sums = call_attend(chunk, place, picks, pieces, moved)
        joined += [by_part(outs[k], k // 2, k % 2, True) for k in range(PARTS)]
        pooled.append(sums)
    attended = call_join_outputs(place, joined)
    pooled = jnp.concatenate(pooled, axis=1).reshape(2, TILES, SHARDS, COMP_PAD)[..., :TILES].reshape(2, TILES, NBLK)
    kept, sent = pooled[0], pooled[1]
    came = by_seq(sent, lambda z, c: to_seq(z, c + 1))
    both = jnp.where(core == 0, jnp.stack([kept, came], axis=1), jnp.stack([came, kept], axis=1))
    factor = (seq * TILES + jnp.arange(TILES, dtype=jnp.int32) + 1).astype(jnp.float32) / (BLOCK * HPG)
    block_scores = (both * factor[:, None, None])[None]
    return block_scores, attended.reshape(1, TOK, 2, GROUPS, DH)


def solution(mesh):
    placed = (
        P("batch", "seq", "head", None, None),
        P("batch", "seq", None, None),
        P("batch", "seq", None, None),
        P("batch", "seq", None, None),
        P("batch", "seq", None, None),
    )
    return jax.shard_map(
        local,
        mesh=mesh,
        in_specs=placed,
        out_specs=(P("batch", "seq", "head", None), P("batch", "seq", "head", None, None)),
        check_vma=False,
    )
```

```python
import functools
import math

import jax
import jax.numpy as jnp
from jax import lax
from jax.experimental import pallas as pl
from jax.experimental.pallas import tpu as pltpu
from jax.sharding import PartitionSpec as P


HPG = 8
GROUPS = 8
DH = 128
BLOCK = 64
TOPN = 16
NBLK = 128
SHARDS = 16
CHIPS = 8
COLS = 4
TOK = 512
TILES = 8
COMP_PAD = 16
PIECE = 2 * TOK + COMP_PAD
PARTS = 8
CHUNKS = 2
TOK_CHUNK = TOK // CHUNKS
TILES_CHUNK = TILES // CHUNKS
KEYS = TOPN * BLOCK
ROWS = HPG * BLOCK
COMP_ROWS = SHARDS * COMP_PAD
STEPS = 4
STEP_BLOCKS = TOPN // STEPS
STEP_KEYS = KEYS // STEPS
STEP_COMP = NBLK // STEPS
ONES = 16
FAR = -1.0e9
EXP2_SCALE = DH**-0.5 * math.log2(math.e)


def iota(shape, dim):
    return lax.broadcasted_iota(jnp.int32, shape, dim)


def dot(lhs, rhs, dims=(((1,), (0,)), ((), ()))):
    return lax.dot_general(lhs, rhs, dims, preferred_element_type=jnp.float32)


def one_hot(cond):
    return jnp.where(cond, 1.0, 0.0).astype(jnp.bfloat16)


def split_pools(place, keys, values, comp, own, other):
    mine = place[0] * 2 + place[1]
    theirs = place[0] * 2 + 1 - place[1]
    step = 32
    row = iota((2 * step, step * GROUPS), 0)
    col = iota((2 * step, step * GROUPS), 1)
    group = jnp.where(row < step, mine, theirs)
    pick = one_hot(col == (row % step) * GROUPS + group)
    for i in range(TOK // step):
        rows = pl.ds(i * step * GROUPS, step * GROUPS)
        both = jnp.concatenate([keys[rows, :], values[rows, :]], axis=1)
        got = dot(pick, both).astype(jnp.bfloat16)
        own[pl.ds(i * step, step), :] = got[:step, :DH]
        own[pl.ds(TOK + i * step, step), :] = got[:step, DH:]
        other[pl.ds(i * step, step), :] = got[step:, :DH]
        other[pl.ds(TOK + i * step, step), :] = got[step:, DH:]
    row = iota((2 * COMP_PAD, TILES * GROUPS), 0)
    col = iota((2 * COMP_PAD, TILES * GROUPS), 1)
    group = jnp.where(row < COMP_PAD, mine, theirs)
    block = row % COMP_PAD
    got = dot(one_hot((col == block * GROUPS + group) & (block < TILES)), comp[...]).astype(jnp.bfloat16)
    own[pl.ds(2 * TOK, COMP_PAD), :] = got[:COMP_PAD]
    other[pl.ds(2 * TOK, COMP_PAD), :] = got[COMP_PAD:]


def row_of(r, place):
    part = r // 32
    head = (r // 16) % 2
    token = r % 16
    group = 2 * ((place[0] + part // 2) % COLS) + (place[1] + part % 2) % 2
    return token * 16 + head * GROUPS + group


def split_queries(tokens, place, queries, *parts):
    shape = (256, 256)
    pick = one_hot(iota(shape, 1) == row_of(iota(shape, 0), place))
    for i in range(tokens // 32):
        pair = jnp.concatenate([queries[pl.ds(i * 512, 256), :], queries[pl.ds(i * 512 + 256, 256), :]], axis=1)
        got = dot(pick, pair).astype(jnp.bfloat16)
        for k in range(PARTS):
            for j in range(2):
                rows = got[k * 32 + j * 16 : k * 32 + j * 16 + 16]
                parts[k][j, pl.ds(i * 32, 16), :] = rows[:, :DH]
                parts[k][j, pl.ds(i * 32 + 16, 16), :] = rows[:, DH:]


def join_outputs(tokens, place, *refs):
    parts, out = refs[:PARTS], refs[-1]
    shape = (256, 256)
    pick = one_hot(iota(shape, 0) == row_of(iota(shape, 1), place))
    for i in range(tokens // 32):
        halves = []
        for h in range(2):
            at = pl.ds(i * 32 + h * 16, 16)
            halves.append(jnp.concatenate([parts[k][j, at, :] for k in range(PARTS) for j in range(2)], axis=0))
        got = dot(pick, jnp.concatenate(halves, axis=1)).astype(jnp.bfloat16)
        out[pl.ds(i * 512, 256), :] = got[:, :DH]
        out[pl.ds(i * 512 + 256, 256), :] = got[:, DH:]


def attend(chunk, place, picks, *refs):
    pieces = refs[: 2 * CHIPS]
    queries = refs[2 * CHIPS : 2 * CHIPS + PARTS]
    outs = refs[2 * CHIPS + PARTS : 2 * CHIPS + 2 * PARTS]
    pooled = refs[2 * CHIPS + 2 * PARTS : 2 * CHIPS + 2 * PARTS + 2]
    pool, comp, mask, *rest, sems = refs[2 * CHIPS + 2 * PARTS + 2 :]
    turned, scores, logits, tops = rest[0:2], rest[2:4], rest[4:6], rest[6:8]
    core, chip = place[1], place[2]
    copies = []
    for k in range(CHIPS):
        for h in range(2):
            slot = 2 * ((chip + k) % CHIPS) + (core + h) % 2
            copies.append(pltpu.make_async_copy(pieces[2 * k + h], pool.at[slot], sems.at[2 * k + h]))
    for copy in copies:
        copy.start()
    shape = (2 * BLOCK, DH)
    row = iota(shape, 0)
    hidden = (row >= BLOCK) & (row - BLOCK > iota(shape, 1))
    mask[...] = jnp.where(hidden, FAR, 0.0).astype(jnp.bfloat16)
    shape = (DH, ROWS)
    for half in range(2):
        turned[half][pl.ds(DH, DH), :] = one_hot(iota(shape, 0) == iota(shape, 1) % BLOCK)
    shape = (NBLK, COMP_ROWS)
    take = one_hot(iota(shape, 1) == iota(shape, 0) // TILES * COMP_PAD + iota(shape, 0) % TILES)
    for copy in copies:
        copy.wait()
    padded = jnp.concatenate([pool[s, pl.ds(2 * TOK, COMP_PAD), :] for s in range(SHARDS)], axis=0)
    comp[...] = dot(take, padded).astype(jnp.bfloat16)
    block_row = iota((NBLK, ROWS), 0)
    ones = jnp.full((ONES, STEP_KEYS), 1.0, jnp.bfloat16)

    def spot(local):
        return pl.ds(pl.multiple_of(local * BLOCK, BLOCK), BLOCK)

    def number_of(local, half):
        return (2 * chip + (core + half) % 2) * TILES + chunk * TILES_CHUNK + local

    def pick_of(local, half, b):
        return picks[(half * TILES + chunk * TILES_CHUNK + local) * TOPN + b]

    def block_of(n, offset):
        return pool[n // TILES, pl.ds(pl.multiple_of(offset + n % TILES * BLOCK, BLOCK), BLOCK), :]

    def turn(local, half):
        at = spot(local)
        query = jnp.concatenate([queries[2 * dx + half][j, at, :] for dx in range(COLS) for j in range(2)], axis=0)
        turned[half][pl.ds(0, DH), :] = query.T

    def score(local, half, i):
        number = number_of(local, half)
        keys = []
        for b in range(STEP_BLOCKS):
            n = pick_of(local, half, i * STEP_BLOCKS + b)
            own = jnp.where(n == number, BLOCK, 0)
            keys.append(jnp.concatenate([block_of(n, 0), mask[pl.ds(pl.multiple_of(own, BLOCK), BLOCK), :]], axis=1))
        some = comp[pl.ds(i * STEP_COMP, STEP_COMP), :]
        keys.append(jnp.concatenate([some, jnp.zeros_like(some)], axis=1))
        got = dot(jnp.concatenate(keys, axis=0), turned[half][...])
        near = got[:STEP_KEYS]
        scores[half][pl.ds(i * STEP_KEYS, STEP_KEYS), :] = near
        logits[half][pl.ds(i * STEP_COMP, STEP_COMP), :] = got[STEP_KEYS:]
        top = jnp.max(near.reshape(STEP_KEYS // 8, 8, ROWS), axis=0)
        tops[half][...] = top if i == 0 else jnp.maximum(tops[half][...], top)

    def weigh(local, half, i, top):
        weight = jnp.exp2((scores[half][pl.ds(i * STEP_KEYS, STEP_KEYS), :] - top) * EXP2_SCALE).astype(jnp.bfloat16)
        blocks = [block_of(pick_of(local, half, i * STEP_BLOCKS + b), TOK) for b in range(STEP_BLOCKS)]
        values = jnp.concatenate([jnp.concatenate(blocks, axis=0).T, ones], axis=0)
        return dot(values, weight)

    def finish(local, half, mixed):
        result = (mixed[:DH] * (1.0 / mixed[DH : DH + 1])).astype(jnp.bfloat16).T
        at = spot(local)
        for dx in range(COLS):
            for j in range(2):
                r = (dx * 2 + j) * BLOCK
                outs[2 * dx + half][j, at, :] = result[r : r + BLOCK]
        number = number_of(local, half)
        known = jnp.where(block_row <= number, logits[half][...], -jnp.inf)
        raised = jnp.exp2((known - jnp.max(known, axis=0, keepdims=True)) * EXP2_SCALE)
        prob = raised * (1.0 / jnp.sum(raised, axis=0, keepdims=True))
        folded = prob[:, :128] + prob[:, 128:256] + prob[:, 256:384] + prob[:, 384:]
        factor = (number + 1).astype(jnp.float32) * (1.0 / (BLOCK * HPG))
        pooled[half][pl.ds(local, 1), :] = jnp.sum(folded.T, axis=0, keepdims=True) * factor

    def pair(this, half, that, other):
        top = jnp.max(tops[half][...], axis=0, keepdims=True)
        mixed = None
        for i in range(STEPS):
            score(that, other, i)
            got = weigh(this, half, i, top)
            mixed = got if mixed is None else mixed + got
        finish(this, half, mixed)

    def step(local, carry):
        following = jnp.minimum(local + 1, TILES_CHUNK - 1)
        pair(local, 0, local, 1)
        turn(following, 0)
        pair(local, 1, following, 0)
        turn(following, 1)
        return carry

    turn(0, 0)
    turn(0, 1)
    for i in range(STEPS):
        score(0, 0, i)
    lax.fori_loop(0, TILES_CHUNK, step, 0)


SMEM = pl.BlockSpec(memory_space=pltpu.SMEM)
VMEM = pl.BlockSpec(memory_space=pltpu.VMEM)
ANY = pl.BlockSpec(memory_space=pl.ANY)


def bf16(*shape):
    return jax.ShapeDtypeStruct(shape, jnp.bfloat16)


def call_split_pools(place, keys, values, comp):
    return pl.pallas_call(
        split_pools,
        in_specs=[SMEM, VMEM, VMEM, VMEM],
        out_specs=[VMEM, VMEM],
        out_shape=[bf16(PIECE, DH)] * 2,
        name="split_pools",
    )(place, keys, values, comp)


def call_split_queries(place, queries):
    steps = 4
    tokens = TOK // steps
    return pl.pallas_call(
        functools.partial(split_queries, tokens),
        grid=(steps,),
        in_specs=[SMEM, pl.BlockSpec((tokens * 16, DH), lambda i: (i, 0))],
        out_specs=[pl.BlockSpec((2, tokens, DH), lambda i: (0, i, 0))] * PARTS,
        out_shape=[bf16(2, TOK, DH)] * PARTS,
        name="split_queries",
    )(place, queries)


def call_attend(chunk, place, picks, pieces, queries):
    return pl.pallas_call(
        functools.partial(attend, chunk),
        grid=(1,),
        in_specs=[SMEM, SMEM]
        + [ANY] * (2 * CHIPS)
        + [pl.BlockSpec((2, TOK_CHUNK, DH), lambda i: (0, chunk, 0))] * PARTS,
        out_specs=[pl.BlockSpec((2, TOK_CHUNK, DH), lambda i: (0, 0, 0))] * PARTS
        + [pl.BlockSpec((TILES_CHUNK, NBLK), lambda i: (0, 0))] * 2,
        out_shape=[bf16(2, TOK_CHUNK, DH)] * PARTS + [jax.ShapeDtypeStruct((TILES_CHUNK, NBLK), jnp.float32)] * 2,
        scratch_shapes=[
            pltpu.VMEM((SHARDS, PIECE, DH), jnp.bfloat16),
            pltpu.VMEM((NBLK, DH), jnp.bfloat16),
            pltpu.VMEM((2 * BLOCK, DH), jnp.bfloat16),
        ]
        + [pltpu.VMEM((2 * DH, ROWS), jnp.bfloat16)] * 2
        + [pltpu.VMEM((KEYS, ROWS), jnp.float32)] * 2
        + [pltpu.VMEM((NBLK, ROWS), jnp.float32)] * 2
        + [pltpu.VMEM((8, ROWS), jnp.float32)] * 2
        + [pltpu.SemaphoreType.DMA((2 * CHIPS,))],
        name="attend",
    )(place, picks, *pieces, *queries)


def call_join_outputs(chunk, place, parts, before):
    extra = [] if before is None else [before]
    return pl.pallas_call(
        functools.partial(join_outputs, TOK_CHUNK),
        grid=(1,),
        in_specs=[SMEM] + [pl.BlockSpec((2, TOK_CHUNK, DH), lambda i: (0, 0, 0))] * PARTS + [ANY] * len(extra),
        out_specs=pl.BlockSpec((TOK_CHUNK * 16, DH), lambda i: (chunk, 0)),
        out_shape=bf16(TOK * 16, DH),
        input_output_aliases={PARTS + 1: 0} if extra else {},
        name="join_outputs",
    )(place, *parts, *extra)


def by_seq(value, move):
    return lax.ppermute(value, "seq", [(s, move(s // 2, s % 2)) for s in range(SHARDS)])


def to_seq(chip, core):
    return chip % CHIPS * 2 + core % 2


def by_part(value, dx, dc, back):
    if dx == 0 and dc == 0:
        return value
    pairs = []
    for s in range(SHARDS):
        for x in range(COLS):
            there = (s ^ dc) * COLS + (x + dx) % COLS
            here = s * COLS + x
            pairs.append((there, here) if back else (here, there))
    return lax.ppermute(value, ("seq", "head"), pairs)


def whole(queries, key_rows, value_rows, compressed, chosen):
    seq = lax.axis_index("seq")
    col = lax.axis_index("head")
    chip, core = seq // 2, seq % 2
    place = jnp.stack([col, core, chip]).astype(jnp.int32)
    own, other = call_split_pools(
        place, key_rows.reshape(TOK * GROUPS, DH), value_rows.reshape(TOK * GROUPS, DH), compressed.reshape(TILES * GROUPS, DH)
    )
    pieces = [None] * (2 * CHIPS)
    pieces[0] = own
    pieces[1] = by_seq(other, lambda z, c: to_seq(z, c + 1))
    up, down = [own, other], [own, other]
    for k in range(1, 4):
        for h in range(2):
            turn = h if k == 1 else 0
            up[h] = by_seq(up[h], lambda z, c: to_seq(z + 1, c + turn))
            down[h] = by_seq(down[h], lambda z, c: to_seq(z - 1, c + turn))
            pieces[2 * (CHIPS - k) + h] = up[h]
            pieces[2 * k + h] = down[h]
    for h in range(2):
        onward = jnp.where(core == 0, up[h], down[h])
        pieces[2 * 4 + h] = by_seq(onward, lambda z, c: to_seq(z + (1 if c == 0 else -1), c))
    parts = call_split_queries(place, queries.reshape(TOK * 16, DH))
    moved = []
    for k in range(PARTS):
        moved.append(by_part(parts[k], k // 2, k % 2, False))
    groups = chosen[0].transpose(1, 0, 2)
    mine = lax.dynamic_index_in_dim(groups, 2 * col + core, 0, False)
    theirs = lax.dynamic_index_in_dim(groups, 2 * col + 1 - core, 0, False)
    theirs = by_seq(theirs, lambda z, c: to_seq(z, c + 1))
    picks = jnp.concatenate([mine, theirs]).reshape(-1)
    attended, kept, came, joined = None, [], [], []
    for chunk in range(CHUNKS):
        *outs, keep, send = call_attend(chunk, place, picks, pieces, moved)
        back = []
        for k in range(PARTS):
            back.append(by_part(outs[k], k // 2, k % 2, True))
        came.append(by_seq(send, lambda z, c: to_seq(z, c + 1)))
        kept.append(keep)
        joined.append(back)
    for chunk in range(CHUNKS):
        attended = call_join_outputs(chunk, place, joined[chunk], attended)
    kept, came = jnp.concatenate(kept), jnp.concatenate(came)
    both = jnp.where(core == 0, jnp.stack([kept, came], axis=1), jnp.stack([came, kept], axis=1))
    return both[None], attended.reshape(1, TOK, 2, GROUPS, DH)


def solution(mesh):
    placed = (
        P("batch", "seq", "head", None, None),
        P("batch", "seq", None, None),
        P("batch", "seq", None, None),
        P("batch", "seq", None, None),
        P("batch", "seq", None, None),
    )
    return jax.shard_map(
        whole,
        mesh=mesh,
        in_specs=placed,
        out_specs=(P("batch", "seq", "head", None), P("batch", "seq", "head", None, None)),
        check_vma=False,
    )
```

```python
import functools
import math

import jax
import jax.numpy as jnp
from jax import lax
from jax.experimental import pallas as pl
from jax.experimental.pallas import tpu as pltpu
from jax.sharding import PartitionSpec as P


HPG = 8
GROUPS = 8
DH = 128
BLOCK = 64
TOPN = 16
NBLK = 128
SHARDS = 16
CHIPS = 8
COLS = 4
TOK = 512
TILES = 8
COMP_PAD = 16
PIECE = 2 * TOK + COMP_PAD
PARTS = 8
POOL_TOK = 128
JOIN_TOK = 64
CHUNKS = ((1, 2), (3, 0))
WIDE = 2
KEYS = TOPN * BLOCK
ROWS = WIDE * 2 * BLOCK
COMP_ROWS = SHARDS * COMP_PAD
STEPS = 4
STEP_BLOCKS = TOPN // STEPS
STEP_KEYS = KEYS // STEPS
STEP_COMP = NBLK // STEPS
ONES = 16
FAR = -1.0e9
EXP2_SCALE = DH**-0.5 * math.log2(math.e)


def iota(shape, dim):
    return lax.broadcasted_iota(jnp.int32, shape, dim)


def dot(lhs, rhs, dims=(((1,), (0,)), ((), ()))):
    return lax.dot_general(lhs, rhs, dims, preferred_element_type=jnp.float32)


def one_hot(cond):
    return jnp.where(cond, 1.0, 0.0).astype(jnp.bfloat16)


def split_pools(place, keys, values, comp, own, other):
    mine = place[0] * 2 + place[1]
    theirs = place[0] * 2 + 1 - place[1]
    step = 32
    row = iota((2 * step, step * GROUPS), 0)
    col = iota((2 * step, step * GROUPS), 1)
    group = jnp.where(row < step, mine, theirs)
    pick = one_hot(col == (row % step) * GROUPS + group)
    base = pl.program_id(0) * POOL_TOK
    for i in range(POOL_TOK // step):
        rows = pl.ds(i * step * GROUPS, step * GROUPS)
        got = dot(pick, jnp.concatenate([keys[rows, :], values[rows, :]], axis=1)).astype(jnp.bfloat16)
        low = pl.ds(pl.multiple_of(base + i * step, step), step)
        high = pl.ds(pl.multiple_of(base + TOK + i * step, step), step)
        own[low, :] = got[:step, :DH]
        own[high, :] = got[:step, DH:]
        other[low, :] = got[step:, :DH]
        other[high, :] = got[step:, DH:]

    @pl.when(pl.program_id(0) == 0)
    def _():
        row = iota((2 * COMP_PAD, TILES * GROUPS), 0)
        col = iota((2 * COMP_PAD, TILES * GROUPS), 1)
        group = jnp.where(row < COMP_PAD, mine, theirs)
        block = row % COMP_PAD
        got = dot(one_hot((col == block * GROUPS + group) & (block < TILES)), comp[...]).astype(jnp.bfloat16)
        own[pl.ds(2 * TOK, COMP_PAD), :] = got[:COMP_PAD]
        other[pl.ds(2 * TOK, COMP_PAD), :] = got[COMP_PAD:]


def row_of(r, place):
    part = r // 32
    head = (r // 16) % 2
    token = r % 16
    group = 2 * ((place[0] + part // 2) % COLS) + (place[1] + part % 2) % 2
    return token * 16 + head * GROUPS + group


def split_queries(tokens, place, queries, *parts):
    shape = (256, 256)
    pick = one_hot(iota(shape, 1) == row_of(iota(shape, 0), place))
    for i in range(tokens // 32):
        pair = jnp.concatenate([queries[pl.ds(i * 512, 256), :], queries[pl.ds(i * 512 + 256, 256), :]], axis=1)
        got = dot(pick, pair).astype(jnp.bfloat16)
        for k in range(PARTS):
            for j in range(2):
                rows = got[k * 32 + j * 16 : k * 32 + j * 16 + 16]
                parts[k][j, pl.ds(i * 32, 16), :] = rows[:, :DH]
                parts[k][j, pl.ds(i * 32 + 16, 16), :] = rows[:, DH:]


def join_outputs(tokens, place, *refs):
    parts, out = refs[:PARTS], refs[-1]
    shape = (256, 256)
    pick = one_hot(iota(shape, 0) == row_of(iota(shape, 1), place))
    for i in range(tokens // 32):
        halves = []
        for h in range(2):
            at = pl.ds(i * 32 + h * 16, 16)
            halves.append(jnp.concatenate([parts[k][j, at, :] for k in range(PARTS) for j in range(2)], axis=0))
        got = dot(pick, jnp.concatenate(halves, axis=1)).astype(jnp.bfloat16)
        out[pl.ds(i * 512, 256), :] = got[:, :DH]
        out[pl.ds(i * 512 + 256, 256), :] = got[:, DH:]


def attend(follows, place, picks, *refs):
    pieces = refs[: 2 * CHIPS]
    refs = refs[2 * CHIPS :]
    count = 2 * WIDE
    queries, refs = refs[:count], refs[count:]
    sofar, refs = (refs[:2], refs[2:]) if follows else (None, refs)
    outs, refs = refs[:count], refs[count:]
    pooled, refs = refs[:2], refs[2:]
    pool, comp, mask, *rest, sems = refs
    turned, scores, logits, tops = rest[0:2], rest[2:4], rest[4:6], rest[6:8]
    core, chip = place[1], place[2]
    copies = []
    for k in range(CHIPS):
        for h in range(2):
            slot = 2 * ((chip + k) % CHIPS) + (core + h) % 2
            copies.append(pltpu.make_async_copy(pieces[2 * k + h], pool.at[slot], sems.at[2 * k + h]))
    for copy in copies:
        copy.start()
    shape = (2 * BLOCK, DH)
    row = iota(shape, 0)
    hidden = (row >= BLOCK) & (row - BLOCK > iota(shape, 1))
    mask[...] = jnp.where(hidden, FAR, 0.0).astype(jnp.bfloat16)
    shape = (DH, ROWS)
    for half in range(2):
        turned[half][pl.ds(DH, DH), :] = one_hot(iota(shape, 0) == iota(shape, 1) % BLOCK)
    shape = (NBLK, COMP_ROWS)
    take = one_hot(iota(shape, 1) == iota(shape, 0) // TILES * COMP_PAD + iota(shape, 0) % TILES)
    for copy in copies:
        copy.wait()
    padded = jnp.concatenate([pool[s, pl.ds(2 * TOK, COMP_PAD), :] for s in range(SHARDS)], axis=0)
    comp[...] = dot(take, padded).astype(jnp.bfloat16)
    block_row = iota((NBLK, ROWS), 0)
    ones = jnp.full((ONES, STEP_KEYS), 1.0, jnp.bfloat16)

    def spot(local):
        return pl.ds(pl.multiple_of(local * BLOCK, BLOCK), BLOCK)

    def number_of(local, half):
        return (2 * chip + (core + half) % 2) * TILES + local

    def pick_of(local, half, b):
        return picks[(half * TILES + local) * TOPN + b]

    def block_of(n, offset):
        return pool[n // TILES, pl.ds(pl.multiple_of(offset + n % TILES * BLOCK, BLOCK), BLOCK), :]

    def turn(local, half):
        at = spot(local)
        query = jnp.concatenate([queries[2 * w + half][j, at, :] for w in range(WIDE) for j in range(2)], axis=0)
        turned[half][pl.ds(0, DH), :] = query.T

    def score(local, half, i):
        number = number_of(local, half)
        keys = []
        for b in range(STEP_BLOCKS):
            n = pick_of(local, half, i * STEP_BLOCKS + b)
            own = jnp.where(n == number, BLOCK, 0)
            keys.append(jnp.concatenate([block_of(n, 0), mask[pl.ds(pl.multiple_of(own, BLOCK), BLOCK), :]], axis=1))
        some = comp[pl.ds(i * STEP_COMP, STEP_COMP), :]
        keys.append(jnp.concatenate([some, jnp.zeros_like(some)], axis=1))
        got = dot(jnp.concatenate(keys, axis=0), turned[half][...])
        near = got[:STEP_KEYS]
        scores[half][pl.ds(i * STEP_KEYS, STEP_KEYS), :] = near
        logits[half][pl.ds(i * STEP_COMP, STEP_COMP), :] = got[STEP_KEYS:]
        top = jnp.max(near.reshape(STEP_KEYS // 8, 8, ROWS), axis=0)
        tops[half][...] = top if i == 0 else jnp.maximum(tops[half][...], top)

    def weigh(local, half, i, top):
        weight = jnp.exp2((scores[half][pl.ds(i * STEP_KEYS, STEP_KEYS), :] - top) * EXP2_SCALE).astype(jnp.bfloat16)
        blocks = [block_of(pick_of(local, half, i * STEP_BLOCKS + b), TOK) for b in range(STEP_BLOCKS)]
        values = jnp.concatenate([jnp.concatenate(blocks, axis=0).T, ones], axis=0)
        return dot(values, weight)

    def finish(local, half, mixed):
        result = (mixed[:DH] * (1.0 / mixed[DH : DH + 1])).astype(jnp.bfloat16).T
        at = spot(local)
        for w in range(WIDE):
            for j in range(2):
                r = (w * 2 + j) * BLOCK
                outs[2 * w + half][j, at, :] = result[r : r + BLOCK]
        number = number_of(local, half)
        known = jnp.where(block_row <= number, logits[half][...], -jnp.inf)
        raised = jnp.exp2((known - jnp.max(known, axis=0, keepdims=True)) * EXP2_SCALE)
        prob = raised * (1.0 / jnp.sum(raised, axis=0, keepdims=True))
        folded = prob[:, :128] + prob[:, 128:]
        factor = (number + 1).astype(jnp.float32) * (1.0 / (BLOCK * HPG))
        sums = jnp.sum(folded.T, axis=0, keepdims=True) * factor
        at = pl.ds(local, 1)
        pooled[half][at, :] = sums + sofar[half][at, :] if follows else sums

    def pair(this, half, that, other):
        top = jnp.max(tops[half][...], axis=0, keepdims=True)
        mixed = None
        for i in range(STEPS):
            score(that, other, i)
            got = weigh(this, half, i, top)
            mixed = got if mixed is None else mixed + got
        finish(this, half, mixed)

    def step(local, carry):
        following = jnp.minimum(local + 1, TILES - 1)
        pair(local, 0, local, 1)
        turn(following, 0)
        pair(local, 1, following, 0)
        turn(following, 1)
        return carry

    turn(0, 0)
    turn(0, 1)
    for i in range(STEPS):
        score(0, 0, i)
    lax.fori_loop(0, TILES, step, 0)


SMEM = pl.BlockSpec(memory_space=pltpu.SMEM)
VMEM = pl.BlockSpec(memory_space=pltpu.VMEM)
ANY = pl.BlockSpec(memory_space=pl.ANY)


def bf16(*shape):
    return jax.ShapeDtypeStruct(shape, jnp.bfloat16)


def call_split_pools(place, keys, values, comp):
    rows = pl.BlockSpec((POOL_TOK * GROUPS, DH), lambda i: (i, 0))
    piece = pl.BlockSpec((PIECE, DH), lambda i: (0, 0))
    return pl.pallas_call(
        split_pools,
        grid=(TOK // POOL_TOK,),
        in_specs=[SMEM, rows, rows, pl.BlockSpec((TILES * GROUPS, DH), lambda i: (0, 0))],
        out_specs=[piece, piece],
        out_shape=[bf16(PIECE, DH)] * 2,
        name="split_pools",
    )(place, keys, values, comp)


def call_split_queries(place, queries):
    steps = 4
    tokens = TOK // steps
    return pl.pallas_call(
        functools.partial(split_queries, tokens),
        grid=(steps,),
        in_specs=[SMEM, pl.BlockSpec((tokens * 16, DH), lambda i: (i, 0))],
        out_specs=[pl.BlockSpec((2, tokens, DH), lambda i: (0, i, 0))] * PARTS,
        out_shape=[bf16(2, TOK, DH)] * PARTS,
        name="split_queries",
    )(place, queries)


def call_attend(chunk, place, picks, pieces, queries, sofar):
    parts = pl.BlockSpec((2, TOK, DH), lambda i: (0, 0, 0))
    sums = pl.BlockSpec((TILES, NBLK), lambda i: (0, 0))
    return pl.pallas_call(
        functools.partial(attend, bool(sofar)),
        grid=(1,),
        in_specs=[SMEM, SMEM] + [ANY] * (2 * CHIPS) + [parts] * (2 * WIDE) + [sums] * len(sofar),
        out_specs=[parts] * (2 * WIDE) + [sums] * 2,
        out_shape=[bf16(2, TOK, DH)] * (2 * WIDE) + [jax.ShapeDtypeStruct((TILES, NBLK), jnp.float32)] * 2,
        scratch_shapes=[
            pltpu.VMEM((SHARDS, PIECE, DH), jnp.bfloat16),
            pltpu.VMEM((NBLK, DH), jnp.bfloat16),
            pltpu.VMEM((2 * BLOCK, DH), jnp.bfloat16),
        ]
        + [pltpu.VMEM((2 * DH, ROWS), jnp.bfloat16)] * 2
        + [pltpu.VMEM((KEYS, ROWS), jnp.float32)] * 2
        + [pltpu.VMEM((NBLK, ROWS), jnp.float32)] * 2
        + [pltpu.VMEM((8, ROWS), jnp.float32)] * 2
        + [pltpu.SemaphoreType.DMA((2 * CHIPS,))],
        name="attend",
    )(place, picks, *pieces, *[queries[2 * dx + half] for dx in chunk for half in range(2)], *sofar)


def call_join_outputs(place, parts):
    return pl.pallas_call(
        functools.partial(join_outputs, JOIN_TOK),
        grid=(TOK // JOIN_TOK,),
        in_specs=[SMEM] + [pl.BlockSpec((2, JOIN_TOK, DH), lambda i: (0, i, 0))] * PARTS,
        out_specs=pl.BlockSpec((JOIN_TOK * 16, DH), lambda i: (i, 0)),
        out_shape=bf16(TOK * 16, DH),
        name="join_outputs",
    )(place, *parts)


def by_seq(value, move):
    return lax.ppermute(value, "seq", [(s, move(s // 2, s % 2)) for s in range(SHARDS)])


def to_seq(chip, core):
    return chip % CHIPS * 2 + core % 2


def by_part(value, dx, dc, back):
    if dx == 0 and dc == 0:
        return value
    pairs = []
    for s in range(SHARDS):
        for x in range(COLS):
            there = (s ^ dc) * COLS + (x + dx) % COLS
            here = s * COLS + x
            pairs.append((there, here) if back else (here, there))
    return lax.ppermute(value, ("seq", "head"), pairs)


def whole(queries, key_rows, value_rows, compressed, chosen):
    seq = lax.axis_index("seq")
    col = lax.axis_index("head")
    chip, core = seq // 2, seq % 2
    place = jnp.stack([col, core, chip]).astype(jnp.int32)
    own, other = call_split_pools(
        place, key_rows.reshape(TOK * GROUPS, DH), value_rows.reshape(TOK * GROUPS, DH), compressed.reshape(TILES * GROUPS, DH)
    )
    pieces = [None] * (2 * CHIPS)
    pieces[0] = own
    pieces[1] = by_seq(other, lambda z, c: to_seq(z, c + 1))
    up, down = [own, other], [own, other]
    for k in range(1, 4):
        for h in range(2):
            turn = h if k == 1 else 0
            up[h] = by_seq(up[h], lambda z, c: to_seq(z + 1, c + turn))
            down[h] = by_seq(down[h], lambda z, c: to_seq(z - 1, c + turn))
            pieces[2 * (CHIPS - k) + h] = up[h]
            pieces[2 * k + h] = down[h]
    pieces[2 * 4] = by_seq(up[0], lambda z, c: to_seq(z + 1, c))
    pieces[2 * 4 + 1] = by_seq(down[1], lambda z, c: to_seq(z - 1, c))
    parts = call_split_queries(place, queries.reshape(TOK * 16, DH))
    moved = []
    for k in range(PARTS):
        moved.append(by_part(parts[k], k // 2, k % 2, False))
    groups = chosen[0].transpose(1, 0, 2)
    mine = lax.dynamic_index_in_dim(groups, 2 * col + core, 0, False)
    theirs = lax.dynamic_index_in_dim(groups, 2 * col + 1 - core, 0, False)
    theirs = by_seq(theirs, lambda z, c: to_seq(z, c + 1))
    picks = jnp.concatenate([mine, theirs]).reshape(-1)
    joined, sums = [None] * PARTS, []
    for chunk in CHUNKS:
        *outs, keep, send = call_attend(chunk, place, picks, pieces, moved, sums)
        sums = [keep, send]
        for w, dx in enumerate(chunk):
            for half in range(2):
                joined[2 * dx + half] = by_part(outs[2 * w + half], dx, half, True)
    came = by_seq(send, lambda z, c: to_seq(z, c + 1))
    attended = call_join_outputs(place, joined)
    both = jnp.where(core == 0, jnp.stack([keep, came], axis=1), jnp.stack([came, keep], axis=1))
    return both[None], attended.reshape(1, TOK, 2, GROUPS, DH)


def solution(mesh):
    placed = (
        P("batch", "seq", "head", None, None),
        P("batch", "seq", None, None),
        P("batch", "seq", None, None),
        P("batch", "seq", None, None),
        P("batch", "seq", None, None),
    )
    return jax.shard_map(
        whole,
        mesh=mesh,
        in_specs=placed,
        out_specs=(P("batch", "seq", "head", None), P("batch", "seq", "head", None, None)),
        check_vma=False,
    )
```

```python
import functools
import math

import jax
import jax.numpy as jnp
from jax import lax
from jax.experimental import pallas as pl
from jax.experimental.pallas import tpu as pltpu
from jax.sharding import PartitionSpec as P


HPG = 8
GROUPS = 8
DH = 128
BLOCK = 64
TOPN = 16
NBLK = 128
SHARDS = 16
CHIPS = 8
COLS = 4
TOK = 512
TILES = 8
COMP_PAD = 16
PIECE = 2 * TOK + COMP_PAD
PARTS = 8
POOL_TOK = 512
JOIN_TOK = 256
CHUNKS = ((1, 2), (3, 0))
WIDE = 2
KEYS = TOPN * BLOCK
ROWS = WIDE * 2 * BLOCK
COMP_ROWS = SHARDS * COMP_PAD
STEPS = 4
STEP_BLOCKS = TOPN // STEPS
STEP_KEYS = KEYS // STEPS
STEP_COMP = NBLK // STEPS
ONES = 16
FAR = -1.0e9
EXP2_SCALE = DH**-0.5 * math.log2(math.e)


def iota(shape, dim):
    return lax.broadcasted_iota(jnp.int32, shape, dim)


def dot(lhs, rhs, dims=(((1,), (0,)), ((), ()))):
    return lax.dot_general(lhs, rhs, dims, preferred_element_type=jnp.float32)


def one_hot(cond):
    return jnp.where(cond, 1.0, 0.0).astype(jnp.bfloat16)


def split_pools(place, keys, values, comp, own, other):
    mine = place[0] * 2 + place[1]
    theirs = place[0] * 2 + 1 - place[1]
    step = 32
    row = iota((2 * step, step * GROUPS), 0)
    col = iota((2 * step, step * GROUPS), 1)
    group = jnp.where(row < step, mine, theirs)
    pick = one_hot(col == (row % step) * GROUPS + group)
    base = pl.program_id(0) * POOL_TOK
    for i in range(POOL_TOK // step):
        rows = pl.ds(i * step * GROUPS, step * GROUPS)
        got = dot(pick, jnp.concatenate([keys[rows, :], values[rows, :]], axis=1)).astype(jnp.bfloat16)
        low = pl.ds(pl.multiple_of(base + i * step, step), step)
        high = pl.ds(pl.multiple_of(base + TOK + i * step, step), step)
        own[low, :] = got[:step, :DH]
        own[high, :] = got[:step, DH:]
        other[low, :] = got[step:, :DH]
        other[high, :] = got[step:, DH:]

    @pl.when(pl.program_id(0) == 0)
    def _():
        row = iota((2 * COMP_PAD, TILES * GROUPS), 0)
        col = iota((2 * COMP_PAD, TILES * GROUPS), 1)
        group = jnp.where(row < COMP_PAD, mine, theirs)
        block = row % COMP_PAD
        got = dot(one_hot((col == block * GROUPS + group) & (block < TILES)), comp[...]).astype(jnp.bfloat16)
        own[pl.ds(2 * TOK, COMP_PAD), :] = got[:COMP_PAD]
        other[pl.ds(2 * TOK, COMP_PAD), :] = got[COMP_PAD:]


def row_of(r, place):
    part = r // 32
    head = (r // 16) % 2
    token = r % 16
    group = 2 * ((place[0] + part // 2) % COLS) + (place[1] + part % 2) % 2
    return token * 16 + head * GROUPS + group


def split_queries(tokens, place, queries, *parts):
    shape = (256, 256)
    pick = one_hot(iota(shape, 1) == row_of(iota(shape, 0), place))
    for i in range(tokens // 32):
        pair = jnp.concatenate([queries[pl.ds(i * 512, 256), :], queries[pl.ds(i * 512 + 256, 256), :]], axis=1)
        got = dot(pick, pair).astype(jnp.bfloat16)
        for k in range(PARTS):
            for j in range(2):
                rows = got[k * 32 + j * 16 : k * 32 + j * 16 + 16]
                parts[k][j, pl.ds(i * 32, 16), :] = rows[:, :DH]
                parts[k][j, pl.ds(i * 32 + 16, 16), :] = rows[:, DH:]


def join_outputs(tokens, place, *refs):
    parts, out = refs[:PARTS], refs[-1]
    shape = (256, 256)
    pick = one_hot(iota(shape, 0) == row_of(iota(shape, 1), place))
    for i in range(tokens // 32):
        halves = []
        for h in range(2):
            at = pl.ds(i * 32 + h * 16, 16)
            halves.append(jnp.concatenate([parts[k][j, at, :] for k in range(PARTS) for j in range(2)], axis=0))
        got = dot(pick, jnp.concatenate(halves, axis=1)).astype(jnp.bfloat16)
        out[pl.ds(i * 512, 256), :] = got[:, :DH]
        out[pl.ds(i * 512 + 256, 256), :] = got[:, DH:]


def attend(follows, place, picks, owns, *refs):
    count = 2 * WIDE
    pieces, refs = refs[: 2 * CHIPS], refs[2 * CHIPS :]
    given, refs = refs[:count], refs[count:]
    sofar, refs = (refs[:2], refs[2:]) if follows else (None, refs)
    outs, refs = refs[:count], refs[count:]
    pooled, refs = refs[:2], refs[2:]
    pool, queries, results, comp, mask, *rest, sems, ask_sems, out_sems = refs
    turned, scores, logits, tops = rest[0:2], rest[2:4], rest[4:6], rest[6:8]
    core, chip = place[1], place[2]
    asks = [pltpu.make_async_copy(given[k], queries.at[k], ask_sems.at[k]) for k in range(count)]
    for copy in asks:
        copy.start()
    copies = []
    for k in range(CHIPS):
        for h in range(2):
            slot = 2 * ((chip + k) % CHIPS) + (core + h) % 2
            rows = pl.ds(pl.multiple_of(slot * PIECE, COMP_PAD), PIECE)
            copies.append(pltpu.make_async_copy(pieces[2 * k + h], pool.at[rows, :], sems.at[2 * k + h]))
    for copy in copies:
        copy.start()
    shape = (2 * BLOCK, DH)
    row = iota(shape, 0)
    hidden = (row >= BLOCK) & (row - BLOCK > iota(shape, 1))
    mask[...] = jnp.where(hidden, FAR, 0.0).astype(jnp.bfloat16)
    shape = (DH, ROWS)
    for half in range(2):
        turned[half][pl.ds(DH, DH), :] = one_hot(iota(shape, 0) == iota(shape, 1) % BLOCK)
    shape = (NBLK, COMP_ROWS)
    take = one_hot(iota(shape, 1) == iota(shape, 0) // TILES * COMP_PAD + iota(shape, 0) % TILES)
    block_row = iota((NBLK, ROWS), 0)
    ones = jnp.full((ONES, STEP_KEYS), 1.0, jnp.bfloat16)

    def spot(local):
        return pl.ds(pl.multiple_of(local * BLOCK, BLOCK), BLOCK)

    def number_of(local, half):
        return (2 * chip + (core + half) % 2) * TILES + local

    def block_of(local, half, b, offset):
        start = picks[(half * TILES + local) * TOPN + b] + offset
        return pool[pl.ds(pl.multiple_of(start, COMP_PAD), BLOCK), :]

    def mask_of(local, half, b):
        start = owns[(half * TILES + local) * TOPN + b]
        return mask[pl.ds(pl.multiple_of(start, BLOCK), BLOCK), :]

    def turn(local, half):
        at = spot(local)
        query = jnp.concatenate([queries[2 * w + half, j, at, :] for w in range(WIDE) for j in range(2)], axis=0)
        turned[half][pl.ds(0, DH), :] = query.T

    def score(local, half, i):
        keys = []
        for b in range(i * STEP_BLOCKS, (i + 1) * STEP_BLOCKS):
            keys.append(jnp.concatenate([block_of(local, half, b, 0), mask_of(local, half, b)], axis=1))
        some = comp[pl.ds(i * STEP_COMP, STEP_COMP), :]
        keys.append(jnp.concatenate([some, jnp.zeros_like(some)], axis=1))
        got = dot(jnp.concatenate(keys, axis=0), turned[half][...])
        near = got[:STEP_KEYS]
        scores[half][pl.ds(i * STEP_KEYS, STEP_KEYS), :] = near
        logits[half][pl.ds(i * STEP_COMP, STEP_COMP), :] = got[STEP_KEYS:]
        return jnp.max(near.reshape(STEP_KEYS // 8, 8, ROWS), axis=0)

    def weigh(local, half, i, top):
        weight = jnp.exp2((scores[half][pl.ds(i * STEP_KEYS, STEP_KEYS), :] - top) * EXP2_SCALE).astype(jnp.bfloat16)
        blocks = [block_of(local, half, b, TOK) for b in range(i * STEP_BLOCKS, (i + 1) * STEP_BLOCKS)]
        values = jnp.concatenate([jnp.concatenate(blocks, axis=0).T, ones], axis=0)
        return dot(values, weight)

    def sending(local, half, w):
        at = spot(local)
        return pltpu.make_async_copy(
            results.at[2 * w + half, :, at, :], outs[2 * w + half].at[:, at, :], out_sems.at[2 * w + half, local]
        )

    def finish(local, half, mixed):
        result = (mixed[:DH] * (1.0 / mixed[DH : DH + 1])).astype(jnp.bfloat16).T
        at = spot(local)
        for w in range(WIDE):
            for j in range(2):
                r = (w * 2 + j) * BLOCK
                results[2 * w + half, j, at, :] = result[r : r + BLOCK]
            sending(local, half, w).start()
        number = number_of(local, half)
        known = jnp.where(block_row <= number, logits[half][...], -jnp.inf)
        raised = jnp.exp2((known - jnp.max(known, axis=0, keepdims=True)) * EXP2_SCALE)
        prob = raised * (1.0 / jnp.sum(raised, axis=0, keepdims=True))
        folded = prob[:, :128] + prob[:, 128:]
        factor = (number + 1).astype(jnp.float32) * (1.0 / (BLOCK * HPG))
        sums = jnp.sum(folded.T, axis=0, keepdims=True) * factor
        at = pl.ds(local, 1)
        pooled[half][at, :] = sums + sofar[half][at, :] if follows else sums

    def pair(this, half, that, other):
        top = jnp.max(tops[half][...], axis=0, keepdims=True)
        mixed, peak = None, None
        for i in range(STEPS):
            near = score(that, other, i)
            peak = near if peak is None else jnp.maximum(peak, near)
            got = weigh(this, half, i, top)
            mixed = got if mixed is None else mixed + got
        tops[other][...] = peak
        finish(this, half, mixed)

    def step(local, carry):
        following = jnp.minimum(local + 1, TILES - 1)
        pair(local, 0, local, 1)
        turn(following, 0)
        pair(local, 1, following, 0)
        turn(following, 1)
        return carry

    for copy in asks:
        copy.wait()
    turn(0, 0)
    turn(0, 1)
    for copy in copies:
        copy.wait()
    padded = [pool[pl.ds(s * PIECE + 2 * TOK, COMP_PAD), :] for s in range(SHARDS)]
    comp[...] = dot(take, jnp.concatenate(padded, axis=0)).astype(jnp.bfloat16)
    peak = score(0, 0, 0)
    for i in range(1, STEPS):
        peak = jnp.maximum(peak, score(0, 0, i))
    tops[0][...] = peak
    lax.fori_loop(0, TILES, step, 0)
    for w in range(WIDE):
        for half in range(2):
            for local in range(TILES):
                sending(local, half, w).wait()


SMEM = pl.BlockSpec(memory_space=pltpu.SMEM)
VMEM = pl.BlockSpec(memory_space=pltpu.VMEM)
ANY = pl.BlockSpec(memory_space=pl.ANY)


def grant(mib):
    return pltpu.CompilerParams(vmem_limit_bytes=mib * 2**20)


def bf16(*shape):
    return jax.ShapeDtypeStruct(shape, jnp.bfloat16)


def call_split_pools(place, keys, values, comp):
    rows = pl.BlockSpec((POOL_TOK * GROUPS, DH), lambda i: (i, 0))
    piece = pl.BlockSpec((PIECE, DH), lambda i: (0, 0))
    return pl.pallas_call(
        split_pools,
        grid=(TOK // POOL_TOK,),
        in_specs=[SMEM, rows, rows, pl.BlockSpec((TILES * GROUPS, DH), lambda i: (0, 0))],
        out_specs=[piece, piece],
        out_shape=[bf16(PIECE, DH)] * 2,
        compiler_params=grant(12),
        name="split_pools",
    )(place, keys, values, comp)


def call_split_queries(place, queries):
    steps = 4
    tokens = TOK // steps
    return pl.pallas_call(
        functools.partial(split_queries, tokens),
        grid=(steps,),
        in_specs=[SMEM, pl.BlockSpec((tokens * 16, DH), lambda i: (i, 0))],
        out_specs=[pl.BlockSpec((2, tokens, DH), lambda i: (0, i, 0))] * PARTS,
        out_shape=[bf16(2, TOK, DH)] * PARTS,
        compiler_params=grant(12),
        name="split_queries",
    )(place, queries)


def call_attend(chunk, place, picks, owns, pieces, queries, sofar):
    return pl.pallas_call(
        functools.partial(attend, bool(sofar)),
        in_specs=[SMEM] * 3 + [ANY] * (2 * CHIPS + 2 * WIDE) + [VMEM] * len(sofar),
        out_specs=[ANY] * (2 * WIDE) + [VMEM] * 2,
        out_shape=[bf16(2, TOK, DH)] * (2 * WIDE) + [jax.ShapeDtypeStruct((TILES, NBLK), jnp.float32)] * 2,
        scratch_shapes=[
            pltpu.VMEM((SHARDS * PIECE, DH), jnp.bfloat16),
            pltpu.VMEM((2 * WIDE, 2, TOK, DH), jnp.bfloat16),
            pltpu.VMEM((2 * WIDE, 2, TOK, DH), jnp.bfloat16),
            pltpu.VMEM((NBLK, DH), jnp.bfloat16),
            pltpu.VMEM((2 * BLOCK, DH), jnp.bfloat16),
        ]
        + [pltpu.VMEM((2 * DH, ROWS), jnp.bfloat16)] * 2
        + [pltpu.VMEM((KEYS, ROWS), jnp.float32)] * 2
        + [pltpu.VMEM((NBLK, ROWS), jnp.float32)] * 2
        + [pltpu.VMEM((8, ROWS), jnp.float32)] * 2
        + [
            pltpu.SemaphoreType.DMA((2 * CHIPS,)),
            pltpu.SemaphoreType.DMA((2 * WIDE,)),
            pltpu.SemaphoreType.DMA((2 * WIDE, TILES)),
        ],
        compiler_params=grant(28),
        name="attend",
    )(place, picks, owns, *pieces, *[queries[2 * dx + half] for dx in chunk for half in range(2)], *sofar)


def call_join_outputs(place, parts):
    return pl.pallas_call(
        functools.partial(join_outputs, JOIN_TOK),
        grid=(TOK // JOIN_TOK,),
        in_specs=[SMEM] + [pl.BlockSpec((2, JOIN_TOK, DH), lambda i: (0, i, 0))] * PARTS,
        out_specs=pl.BlockSpec((JOIN_TOK * 16, DH), lambda i: (i, 0)),
        out_shape=bf16(TOK * 16, DH),
        compiler_params=grant(12),
        name="join_outputs",
    )(place, *parts)


def by_seq(value, move):
    return lax.ppermute(value, "seq", [(s, move(s // 2, s % 2)) for s in range(SHARDS)])


def to_seq(chip, core):
    return chip % CHIPS * 2 + core % 2


def by_part(value, dx, dc, back):
    if dx == 0 and dc == 0:
        return value
    pairs = []
    for s in range(SHARDS):
        for x in range(COLS):
            there = (s ^ dc) * COLS + (x + dx) % COLS
            here = s * COLS + x
            pairs.append((there, here) if back else (here, there))
    return lax.ppermute(value, ("seq", "head"), pairs)


def whole(queries, key_rows, value_rows, compressed, chosen):
    seq = lax.axis_index("seq")
    col = lax.axis_index("head")
    chip, core = seq // 2, seq % 2
    place = jnp.stack([col, core, chip]).astype(jnp.int32)
    own, other = call_split_pools(
        place, key_rows.reshape(TOK * GROUPS, DH), value_rows.reshape(TOK * GROUPS, DH), compressed.reshape(TILES * GROUPS, DH)
    )
    pieces = [None] * (2 * CHIPS)
    pieces[0] = own
    pieces[1] = by_seq(other, lambda z, c: to_seq(z, c + 1))
    up, down = [own, other], [own, other]
    for k in range(1, 4):
        for h in range(2):
            turn = h if k == 1 else 0
            up[h] = by_seq(up[h], lambda z, c: to_seq(z + 1, c + turn))
            down[h] = by_seq(down[h], lambda z, c: to_seq(z - 1, c + turn))
            pieces[2 * (CHIPS - k) + h] = up[h]
            pieces[2 * k + h] = down[h]
    pieces[2 * 4] = by_seq(up[0], lambda z, c: to_seq(z + 1, c))
    pieces[2 * 4 + 1] = by_seq(down[1], lambda z, c: to_seq(z - 1, c))
    parts = call_split_queries(place, queries.reshape(TOK * 16, DH))
    moved = []
    for k in range(PARTS):
        moved.append(by_part(parts[k], k // 2, k % 2, False))
    groups = chosen[0].transpose(1, 0, 2)
    mine = lax.dynamic_index_in_dim(groups, 2 * col + core, 0, False)
    theirs = lax.dynamic_index_in_dim(groups, 2 * col + 1 - core, 0, False)
    theirs = by_seq(theirs, lambda z, c: to_seq(z, c + 1))
    blocks = jnp.stack([mine, theirs])
    shard = 2 * chip + (core + jnp.arange(2, dtype=jnp.int32)) % 2
    number = shard[:, None] * TILES + jnp.arange(TILES, dtype=jnp.int32)
    picks = (blocks // TILES * PIECE + blocks % TILES * BLOCK).reshape(-1)
    owns = jnp.where(blocks == number[..., None], BLOCK, 0).reshape(-1)
    joined, sums = [None] * PARTS, []
    for chunk in CHUNKS:
        *outs, keep, send = call_attend(chunk, place, picks, owns, pieces, moved, sums)
        sums = [keep, send]
        for w, dx in enumerate(chunk):
            for half in range(2):
                joined[2 * dx + half] = by_part(outs[2 * w + half], dx, half, True)
    came = by_seq(send, lambda z, c: to_seq(z, c + 1))
    attended = call_join_outputs(place, joined)
    both = jnp.where(core == 0, jnp.stack([keep, came], axis=1), jnp.stack([came, keep], axis=1))
    return both[None], attended.reshape(1, TOK, 2, GROUPS, DH)


def solution(mesh):
    placed = (
        P("batch", "seq", "head", None, None),
        P("batch", "seq", None, None),
        P("batch", "seq", None, None),
        P("batch", "seq", None, None),
        P("batch", "seq", None, None),
    )
    return jax.shard_map(
        whole,
        mesh=mesh,
        in_specs=placed,
        out_specs=(P("batch", "seq", "head", None), P("batch", "seq", "head", None, None)),
        check_vma=False,
    )
```

```python
import functools
import math

import jax
import jax.numpy as jnp
from jax import lax
from jax.experimental import pallas as pl
from jax.experimental.pallas import tpu as pltpu
from jax.sharding import PartitionSpec as P


HPG = 8
GROUPS = 8
DH = 128
BLOCK = 64
TOPN = 16
NBLK = 128
SHARDS = 16
CHIPS = 8
COLS = 4
TOK = 512
TILES = 8
COMP_PAD = 16
PIECE = 2 * TOK + COMP_PAD
PARTS = 8
LOADS = 4
HALVES = (1, 0)
KEYS = TOPN * BLOCK
ROWS = HPG * BLOCK
COMP_ROWS = SHARDS * COMP_PAD
STEPS = 4
STEP_BLOCKS = TOPN // STEPS
STEP_KEYS = KEYS // STEPS
STEP_COMP = NBLK // STEPS
ONES = 16
FAR = -1.0e9
EXP2_SCALE = DH**-0.5 * math.log2(math.e)


def iota(shape, dim):
    return lax.broadcasted_iota(jnp.int32, shape, dim)


def dot(lhs, rhs, dims=(((1,), (0,)), ((), ()))):
    return lax.dot_general(lhs, rhs, dims, preferred_element_type=jnp.float32)


def one_hot(cond):
    return jnp.where(cond, 1.0, 0.0).astype(jnp.bfloat16)


def split_pools(place, keys, values, comp, own, other, stage, sems):
    mine = place[0] * 2 + place[1]
    theirs = place[0] * 2 + 1 - place[1]
    size = TOK * GROUPS // LOADS
    copies = []
    for i in range(LOADS):
        rows = pl.ds(i * size, size)
        copies.append([pltpu.make_async_copy(ref.at[rows, :], stage.at[k, rows, :], sems.at[k, i]) for k, ref in enumerate((keys, values))])
    for pair in copies:
        for copy in pair:
            copy.start()
    step = 32
    row = iota((2 * step, step * GROUPS), 0)
    col = iota((2 * step, step * GROUPS), 1)
    group = jnp.where(row < step, mine, theirs)
    pick = one_hot(col == (row % step) * GROUPS + group)
    row = iota((2 * COMP_PAD, TILES * GROUPS), 0)
    col = iota((2 * COMP_PAD, TILES * GROUPS), 1)
    group = jnp.where(row < COMP_PAD, mine, theirs)
    block = row % COMP_PAD
    got = dot(one_hot((col == block * GROUPS + group) & (block < TILES)), comp[...]).astype(jnp.bfloat16)
    own[pl.ds(2 * TOK, COMP_PAD), :] = got[:COMP_PAD]
    other[pl.ds(2 * TOK, COMP_PAD), :] = got[COMP_PAD:]
    for i in range(TOK // step):
        if i % (TOK // step // LOADS) == 0:
            for copy in copies[i // (TOK // step // LOADS)]:
                copy.wait()
        rows = pl.ds(i * step * GROUPS, step * GROUPS)
        got = dot(pick, jnp.concatenate([stage[0, rows, :], stage[1, rows, :]], axis=1)).astype(jnp.bfloat16)
        own[pl.ds(i * step, step), :] = got[:step, :DH]
        own[pl.ds(TOK + i * step, step), :] = got[:step, DH:]
        other[pl.ds(i * step, step), :] = got[step:, :DH]
        other[pl.ds(TOK + i * step, step), :] = got[step:, DH:]


def row_of(r, place):
    part = r // 32
    head = (r // 16) % 2
    token = r % 16
    group = 2 * ((place[0] + part // 2) % COLS) + (place[1] + part % 2) % 2
    return token * 16 + head * GROUPS + group


def split_queries(tokens, place, queries, *parts):
    shape = (256, 256)
    pick = one_hot(iota(shape, 1) == row_of(iota(shape, 0), place))
    for i in range(tokens // 32):
        pair = jnp.concatenate([queries[pl.ds(i * 512, 256), :], queries[pl.ds(i * 512 + 256, 256), :]], axis=1)
        got = dot(pick, pair).astype(jnp.bfloat16)
        for k in range(PARTS):
            for j in range(2):
                rows = got[k * 32 + j * 16 : k * 32 + j * 16 + 16]
                parts[k][j, pl.ds(i * 32, 16), :] = rows[:, :DH]
                parts[k][j, pl.ds(i * 32 + 16, 16), :] = rows[:, DH:]


def join_outputs(place, *refs):
    parts, (out, result, sems) = refs[:PARTS], refs[PARTS:]
    shape = (256, 256)
    pick = one_hot(iota(shape, 0) == row_of(iota(shape, 1), place))
    copies = []
    for i in range(TOK // 32):
        halves = []
        for h in range(2):
            at = pl.ds(i * 32 + h * 16, 16)
            halves.append(jnp.concatenate([parts[k][j, at, :] for k in range(PARTS) for j in range(2)], axis=0))
        got = dot(pick, jnp.concatenate(halves, axis=1)).astype(jnp.bfloat16)
        result[pl.ds(i * 512, 256), :] = got[:, :DH]
        result[pl.ds(i * 512 + 256, 256), :] = got[:, DH:]
        if i % 4 == 3:
            rows = pl.ds((i - 3) * 512, 2048)
            copies.append(pltpu.make_async_copy(result.at[rows, :], out.at[rows, :], sems.at[i // 4]))
            copies[-1].start()
    for copy in copies:
        copy.wait()


def attend(half, place, picks, owns, *refs):
    pieces, refs = refs[: 2 * CHIPS], refs[2 * CHIPS :]
    queries, refs = refs[:COLS], refs[COLS:]
    outs, refs = refs[:COLS], refs[COLS:]
    pooled, pool, comp, mask, *rest, sems = refs
    turned, scores, logits, tops = rest[0:2], rest[2:4], rest[4:6], rest[6:8]
    core, chip = place[1], place[2]
    copies = []
    for k in range(CHIPS):
        for h in range(2):
            slot = 2 * ((chip + k) % CHIPS) + (core + h) % 2
            rows = pl.ds(pl.multiple_of(slot * PIECE, COMP_PAD), PIECE)
            copies.append(pltpu.make_async_copy(pieces[2 * k + h], pool.at[rows, :], sems.at[2 * k + h]))
    for copy in copies:
        copy.start()
    shape = (2 * BLOCK, DH)
    row = iota(shape, 0)
    hidden = (row >= BLOCK) & (row - BLOCK > iota(shape, 1))
    mask[...] = jnp.where(hidden, FAR, 0.0).astype(jnp.bfloat16)
    shape = (DH, ROWS)
    for stream in range(2):
        turned[stream][pl.ds(DH, DH), :] = one_hot(iota(shape, 0) == iota(shape, 1) % BLOCK)
    shape = (NBLK, COMP_ROWS)
    take = one_hot(iota(shape, 1) == iota(shape, 0) // TILES * COMP_PAD + iota(shape, 0) % TILES)
    block_row = iota((NBLK, ROWS), 0)
    ones = jnp.full((ONES, STEP_KEYS), 1.0, jnp.bfloat16)

    def spot(local):
        return pl.ds(pl.multiple_of(local * BLOCK, BLOCK), BLOCK)

    def block_of(local, b, offset):
        start = picks[(half * TILES + local) * TOPN + b] + offset
        return pool[pl.ds(pl.multiple_of(start, COMP_PAD), BLOCK), :]

    def mask_of(local, b):
        start = owns[(half * TILES + local) * TOPN + b]
        return mask[pl.ds(pl.multiple_of(start, BLOCK), BLOCK), :]

    def turn(local, stream):
        at = spot(local)
        query = jnp.concatenate([queries[dx][j, at, :] for dx in range(COLS) for j in range(2)], axis=0)
        turned[stream][pl.ds(0, DH), :] = query.T

    def score(local, stream, i):
        keys = []
        for b in range(i * STEP_BLOCKS, (i + 1) * STEP_BLOCKS):
            keys.append(jnp.concatenate([block_of(local, b, 0), mask_of(local, b)], axis=1))
        some = comp[pl.ds(i * STEP_COMP, STEP_COMP), :]
        keys.append(jnp.concatenate([some, jnp.zeros_like(some)], axis=1))
        got = dot(jnp.concatenate(keys, axis=0), turned[stream][...])
        near = got[:STEP_KEYS]
        scores[stream][pl.ds(i * STEP_KEYS, STEP_KEYS), :] = near
        logits[stream][pl.ds(i * STEP_COMP, STEP_COMP), :] = got[STEP_KEYS:]
        return jnp.max(near.reshape(STEP_KEYS // 8, 8, ROWS), axis=0)

    def weigh(local, stream, i, top):
        weight = jnp.exp2((scores[stream][pl.ds(i * STEP_KEYS, STEP_KEYS), :] - top) * EXP2_SCALE).astype(jnp.bfloat16)
        blocks = [block_of(local, b, TOK) for b in range(i * STEP_BLOCKS, (i + 1) * STEP_BLOCKS)]
        values = jnp.concatenate([jnp.concatenate(blocks, axis=0).T, ones], axis=0)
        return dot(values, weight)

    def finish(local, stream, mixed):
        result = (mixed[:DH] * (1.0 / mixed[DH : DH + 1])).astype(jnp.bfloat16).T
        at = spot(local)
        for dx in range(COLS):
            for j in range(2):
                r = (dx * 2 + j) * BLOCK
                outs[dx][j, at, :] = result[r : r + BLOCK]
        number = (2 * chip + (core + half) % 2) * TILES + local
        known = jnp.where(block_row <= number, logits[stream][...], -jnp.inf)
        raised = jnp.exp2((known - jnp.max(known, axis=0, keepdims=True)) * EXP2_SCALE)
        prob = raised * (1.0 / jnp.sum(raised, axis=0, keepdims=True))
        folded = prob[:, :128] + prob[:, 128:256] + prob[:, 256:384] + prob[:, 384:]
        factor = (number + 1).astype(jnp.float32) * (1.0 / (BLOCK * HPG))
        pooled[pl.ds(local, 1), :] = jnp.sum(folded.T, axis=0, keepdims=True) * factor

    def pair(this, stream, that, other):
        top = jnp.max(tops[stream][...], axis=0, keepdims=True)
        mixed, peak = None, None
        for i in range(STEPS):
            near = score(that, other, i)
            peak = near if peak is None else jnp.maximum(peak, near)
            got = weigh(this, stream, i, top)
            mixed = got if mixed is None else mixed + got
        tops[other][...] = peak
        finish(this, stream, mixed)

    def step(i, carry):
        even = 2 * i
        pair(even, 0, even + 1, 1)
        turn(jnp.minimum(even + 2, TILES - 2), 0)
        pair(even + 1, 1, jnp.minimum(even + 2, TILES - 2), 0)
        turn(jnp.minimum(even + 3, TILES - 1), 1)
        return carry

    turn(0, 0)
    turn(1, 1)
    for copy in copies:
        copy.wait()
    padded = [pool[pl.ds(s * PIECE + 2 * TOK, COMP_PAD), :] for s in range(SHARDS)]
    comp[...] = dot(take, jnp.concatenate(padded, axis=0)).astype(jnp.bfloat16)
    peak = score(0, 0, 0)
    for i in range(1, STEPS):
        peak = jnp.maximum(peak, score(0, 0, i))
    tops[0][...] = peak
    lax.fori_loop(0, TILES // 2, step, 0)


SMEM = pl.BlockSpec(memory_space=pltpu.SMEM)
VMEM = pl.BlockSpec(memory_space=pltpu.VMEM)
ANY = pl.BlockSpec(memory_space=pl.ANY)


def grant(mib):
    return pltpu.CompilerParams(vmem_limit_bytes=mib * 2**20)


def bf16(*shape):
    return jax.ShapeDtypeStruct(shape, jnp.bfloat16)


def call_split_pools(place, keys, values, comp):
    return pl.pallas_call(
        split_pools,
        in_specs=[SMEM, ANY, ANY, VMEM],
        out_specs=[VMEM, VMEM],
        out_shape=[bf16(PIECE, DH)] * 2,
        scratch_shapes=[pltpu.VMEM((2, TOK * GROUPS, DH), jnp.bfloat16), pltpu.SemaphoreType.DMA((2, LOADS))],
        name="split_pools",
    )(place, keys, values, comp)


def call_split_queries(place, queries):
    steps = 4
    tokens = TOK // steps
    return pl.pallas_call(
        functools.partial(split_queries, tokens),
        grid=(steps,),
        in_specs=[SMEM, pl.BlockSpec((tokens * 16, DH), lambda i: (i, 0))],
        out_specs=[pl.BlockSpec((2, tokens, DH), lambda i: (0, i, 0))] * PARTS,
        out_shape=[bf16(2, TOK, DH)] * PARTS,
        name="split_queries",
    )(place, queries)


def call_attend(half, place, picks, owns, pieces, queries):
    return pl.pallas_call(
        functools.partial(attend, half),
        in_specs=[SMEM] * 3 + [ANY] * (2 * CHIPS) + [VMEM] * COLS,
        out_specs=[VMEM] * (COLS + 1),
        out_shape=[bf16(2, TOK, DH)] * COLS + [jax.ShapeDtypeStruct((TILES, NBLK), jnp.float32)],
        scratch_shapes=[
            pltpu.VMEM((SHARDS * PIECE, DH), jnp.bfloat16),
            pltpu.VMEM((NBLK, DH), jnp.bfloat16),
            pltpu.VMEM((2 * BLOCK, DH), jnp.bfloat16),
        ]
        + [pltpu.VMEM((2 * DH, ROWS), jnp.bfloat16)] * 2
        + [pltpu.VMEM((KEYS, ROWS), jnp.float32)] * 2
        + [pltpu.VMEM((NBLK, ROWS), jnp.float32)] * 2
        + [pltpu.VMEM((8, ROWS), jnp.float32)] * 2
        + [pltpu.SemaphoreType.DMA((2 * CHIPS,))],
        compiler_params=grant(28),
        name="attend",
    )(place, picks, owns, *pieces, *[queries[2 * dx + half] for dx in range(COLS)])


def call_join_outputs(place, parts):
    return pl.pallas_call(
        join_outputs,
        in_specs=[SMEM] + [VMEM] * PARTS,
        out_specs=ANY,
        out_shape=bf16(TOK * 16, DH),
        scratch_shapes=[pltpu.VMEM((TOK * 16, DH), jnp.bfloat16), pltpu.SemaphoreType.DMA((TOK // 128,))],
        compiler_params=grant(16),
        name="join_outputs",
    )(place, *parts)


def by_seq(value, move):
    return lax.ppermute(value, "seq", [(s, move(s // 2, s % 2)) for s in range(SHARDS)])


def to_seq(chip, core):
    return chip % CHIPS * 2 + core % 2


def by_part(value, dx, dc, back):
    if dx == 0 and dc == 0:
        return value
    pairs = []
    for s in range(SHARDS):
        for x in range(COLS):
            there = (s ^ dc) * COLS + (x + dx) % COLS
            here = s * COLS + x
            pairs.append((there, here) if back else (here, there))
    return lax.ppermute(value, ("seq", "head"), pairs)


def whole(queries, key_rows, value_rows, compressed, chosen):
    seq = lax.axis_index("seq")
    col = lax.axis_index("head")
    chip, core = seq // 2, seq % 2
    place = jnp.stack([col, core, chip]).astype(jnp.int32)
    own, other = call_split_pools(
        place, key_rows.reshape(TOK * GROUPS, DH), value_rows.reshape(TOK * GROUPS, DH), compressed.reshape(TILES * GROUPS, DH)
    )
    pieces = [None] * (2 * CHIPS)
    pieces[0] = own
    pieces[1] = by_seq(other, lambda z, c: to_seq(z, c + 1))
    up, down = [own, other], [own, other]
    for k in range(1, 4):
        for h in range(2):
            turn = h if k == 1 else 0
            up[h] = by_seq(up[h], lambda z, c: to_seq(z + 1, c + turn))
            down[h] = by_seq(down[h], lambda z, c: to_seq(z - 1, c + turn))
            pieces[2 * (CHIPS - k) + h] = up[h]
            pieces[2 * k + h] = down[h]
    pieces[2 * 4] = by_seq(up[0], lambda z, c: to_seq(z + 1, c))
    pieces[2 * 4 + 1] = by_seq(down[1], lambda z, c: to_seq(z - 1, c))
    parts = call_split_queries(place, queries.reshape(TOK * 16, DH))
    moved = []
    for k in range(PARTS):
        moved.append(by_part(parts[k], k // 2, k % 2, False))
    groups = chosen[0].transpose(1, 0, 2)
    mine = lax.dynamic_index_in_dim(groups, 2 * col + core, 0, False)
    theirs = lax.dynamic_index_in_dim(groups, 2 * col + 1 - core, 0, False)
    theirs = by_seq(theirs, lambda z, c: to_seq(z, c + 1))
    blocks = jnp.stack([mine, theirs])
    shard = 2 * chip + (core + jnp.arange(2, dtype=jnp.int32)) % 2
    number = shard[:, None] * TILES + jnp.arange(TILES, dtype=jnp.int32)
    picks = (blocks // TILES * PIECE + blocks % TILES * BLOCK).reshape(-1)
    owns = jnp.where(blocks == number[..., None], BLOCK, 0).reshape(-1)
    joined, sums = [None] * PARTS, [None] * 2
    for half in HALVES:
        *outs, sums[half] = call_attend(half, place, picks, owns, pieces, moved)
        for dx in (2, 1, 3, 0):
            joined[2 * dx + half] = by_part(outs[dx], dx, half, True)
    came = by_seq(sums[1], lambda z, c: to_seq(z, c + 1))
    attended = call_join_outputs(place, joined)
    keep = sums[0]
    both = jnp.where(core == 0, jnp.stack([keep, came], axis=1), jnp.stack([came, keep], axis=1))
    return both[None], attended.reshape(1, TOK, 2, GROUPS, DH)


def solution(mesh):
    placed = (
        P("batch", "seq", "head", None, None),
        P("batch", "seq", None, None),
        P("batch", "seq", None, None),
        P("batch", "seq", None, None),
        P("batch", "seq", None, None),
    )
    return jax.shard_map(
        whole,
        mesh=mesh,
        in_specs=placed,
        out_specs=(P("batch", "seq", "head", None), P("batch", "seq", "head", None, None)),
        check_vma=False,
    )
```

```python
import functools
import math

import jax
import jax.numpy as jnp
from jax import lax
from jax.experimental import pallas as pl
from jax.experimental.pallas import tpu as pltpu
from jax.sharding import PartitionSpec as P


HPG = 8
GROUPS = 8
DH = 128
BLOCK = 64
TOPN = 16
NBLK = 128
SHARDS = 16
CHIPS = 8
COLS = 4
TOK = 512
TILES = 8
COMP_PAD = 16
PIECE = 2 * TOK + COMP_PAD
PARTS = 8
CHUNKS = ((1, 0, 8), (0, 0, 6), (0, 6, 2))
KEYS = TOPN * BLOCK
ROWS = HPG * BLOCK
COMP_ROWS = SHARDS * COMP_PAD
STEPS = 4
STEP_BLOCKS = TOPN // STEPS
STEP_KEYS = KEYS // STEPS
STEP_COMP = NBLK // STEPS
ONES = 16
FAR = -1.0e9
EXP2_SCALE = DH**-0.5 * math.log2(math.e)


def iota(shape, dim):
    return lax.broadcasted_iota(jnp.int32, shape, dim)


def dot(lhs, rhs, dims=(((1,), (0,)), ((), ()))):
    return lax.dot_general(lhs, rhs, dims, preferred_element_type=jnp.float32)


def one_hot(cond):
    return jnp.where(cond, 1.0, 0.0).astype(jnp.bfloat16)


def split_pools(place, keys, values, comp, own, other):
    mine = place[0] * 2 + place[1]
    theirs = place[0] * 2 + 1 - place[1]
    step = 32
    row = iota((2 * step, step * GROUPS), 0)
    col = iota((2 * step, step * GROUPS), 1)
    group = jnp.where(row < step, mine, theirs)
    pick = one_hot(col == (row % step) * GROUPS + group)
    for i in range(TOK // step):
        rows = pl.ds(i * step * GROUPS, step * GROUPS)
        both = jnp.concatenate([keys[rows, :], values[rows, :]], axis=1)
        got = dot(pick, both).astype(jnp.bfloat16)
        own[pl.ds(i * step, step), :] = got[:step, :DH]
        own[pl.ds(TOK + i * step, step), :] = got[:step, DH:]
        other[pl.ds(i * step, step), :] = got[step:, :DH]
        other[pl.ds(TOK + i * step, step), :] = got[step:, DH:]
    row = iota((2 * COMP_PAD, TILES * GROUPS), 0)
    col = iota((2 * COMP_PAD, TILES * GROUPS), 1)
    group = jnp.where(row < COMP_PAD, mine, theirs)
    block = row % COMP_PAD
    got = dot(one_hot((col == block * GROUPS + group) & (block < TILES)), comp[...]).astype(jnp.bfloat16)
    own[pl.ds(2 * TOK, COMP_PAD), :] = got[:COMP_PAD]
    other[pl.ds(2 * TOK, COMP_PAD), :] = got[COMP_PAD:]


def row_of(r, place):
    part = r // 32
    head = (r // 16) % 2
    token = r % 16
    group = 2 * ((place[0] + part // 2) % COLS) + (place[1] + part % 2) % 2
    return token * 16 + head * GROUPS + group


def split_queries(tokens, place, queries, *parts):
    shape = (256, 256)
    pick = one_hot(iota(shape, 1) == row_of(iota(shape, 0), place))
    for i in range(tokens // 32):
        pair = jnp.concatenate([queries[pl.ds(i * 512, 256), :], queries[pl.ds(i * 512 + 256, 256), :]], axis=1)
        got = dot(pick, pair).astype(jnp.bfloat16)
        for k in range(PARTS):
            for j in range(2):
                rows = got[k * 32 + j * 16 : k * 32 + j * 16 + 16]
                parts[k][j, pl.ds(i * 32, 16), :] = rows[:, :DH]
                parts[k][j, pl.ds(i * 32 + 16, 16), :] = rows[:, DH:]


def join_outputs(place, *refs):
    *parts, out, result, sems = refs
    chunks = [parts[c * COLS : (c + 1) * COLS] for c in range(len(CHUNKS))]

    def some(k, j, token):
        for (half, begin, count), group in zip(CHUNKS, chunks):
            at = token - begin * BLOCK
            if half == k % 2 and 0 <= at < count * BLOCK:
                return group[k // 2][j, pl.ds(at, 16), :]

    shape = (256, 256)
    pick = one_hot(iota(shape, 0) == row_of(iota(shape, 1), place))
    copies = []
    for i in range(TOK // 32):
        halves = []
        for h in range(2):
            token = i * 32 + h * 16
            halves.append(jnp.concatenate([some(k, j, token) for k in range(PARTS) for j in range(2)], axis=0))
        got = dot(pick, jnp.concatenate(halves, axis=1)).astype(jnp.bfloat16)
        result[pl.ds(i * 512, 256), :] = got[:, :DH]
        result[pl.ds(i * 512 + 256, 256), :] = got[:, DH:]
        if i % 4 == 3:
            rows = pl.ds((i - 3) * 512, 2048)
            copies.append(pltpu.make_async_copy(result.at[rows, :], out.at[rows, :], sems.at[i // 4]))
            copies[-1].start()
    for copy in copies:
        copy.wait()


def attend(half, begin, count, place, picks, owns, *refs):
    pieces, refs = refs[: 2 * CHIPS], refs[2 * CHIPS :]
    queries, refs = refs[:COLS], refs[COLS:]
    outs, refs = refs[:COLS], refs[COLS:]
    pooled, pool, comp, mask, *rest, sems = refs
    turned, scores, logits, tops = rest[0:2], rest[2:4], rest[4:6], rest[6:8]
    core, chip = place[1], place[2]
    copies = []
    for k in range(CHIPS):
        for h in range(2):
            slot = 2 * ((chip + k) % CHIPS) + (core + h) % 2
            rows = pl.ds(pl.multiple_of(slot * PIECE, COMP_PAD), PIECE)
            copies.append(pltpu.make_async_copy(pieces[2 * k + h], pool.at[rows, :], sems.at[2 * k + h]))
    for copy in copies:
        copy.start()
    shape = (2 * BLOCK, DH)
    row = iota(shape, 0)
    hidden = (row >= BLOCK) & (row - BLOCK > iota(shape, 1))
    mask[...] = jnp.where(hidden, FAR, 0.0).astype(jnp.bfloat16)
    shape = (DH, ROWS)
    for stream in range(2):
        turned[stream][pl.ds(DH, DH), :] = one_hot(iota(shape, 0) == iota(shape, 1) % BLOCK)
    shape = (NBLK, COMP_ROWS)
    take = one_hot(iota(shape, 1) == iota(shape, 0) // TILES * COMP_PAD + iota(shape, 0) % TILES)
    block_row = iota((NBLK, ROWS), 0)
    ones = jnp.full((ONES, STEP_KEYS), 1.0, jnp.bfloat16)

    def spot(local):
        return pl.ds(local * BLOCK if isinstance(local, int) else pl.multiple_of(local * BLOCK, BLOCK), BLOCK)

    def block_of(local, b, offset):
        start = picks[(half * TILES + local) * TOPN + b] + offset
        return pool[pl.ds(pl.multiple_of(start, COMP_PAD), BLOCK), :]

    def mask_of(local, b):
        start = owns[(half * TILES + local) * TOPN + b]
        return mask[pl.ds(pl.multiple_of(start, BLOCK), BLOCK), :]

    def turn(local, stream):
        at = spot(local)
        query = jnp.concatenate([queries[dx][j, at, :] for dx in range(COLS) for j in range(2)], axis=0)
        turned[stream][pl.ds(0, DH), :] = query.T

    def score(local, stream, i):
        keys = []
        for b in range(i * STEP_BLOCKS, (i + 1) * STEP_BLOCKS):
            keys.append(jnp.concatenate([block_of(local, b, 0), mask_of(local, b)], axis=1))
        some = comp[pl.ds(i * STEP_COMP, STEP_COMP), :]
        keys.append(jnp.concatenate([some, jnp.zeros_like(some)], axis=1))
        got = dot(jnp.concatenate(keys, axis=0), turned[stream][...])
        near = got[:STEP_KEYS]
        scores[stream][pl.ds(i * STEP_KEYS, STEP_KEYS), :] = near
        logits[stream][pl.ds(i * STEP_COMP, STEP_COMP), :] = got[STEP_KEYS:]
        return jnp.max(near.reshape(STEP_KEYS // 8, 8, ROWS), axis=0)

    def weigh(local, stream, i, top):
        weight = jnp.exp2((scores[stream][pl.ds(i * STEP_KEYS, STEP_KEYS), :] - top) * EXP2_SCALE).astype(jnp.bfloat16)
        blocks = [block_of(local, b, TOK) for b in range(i * STEP_BLOCKS, (i + 1) * STEP_BLOCKS)]
        values = jnp.concatenate([jnp.concatenate(blocks, axis=0).T, ones], axis=0)
        return dot(values, weight)

    def finish(local, stream, mixed):
        result = (mixed[:DH] * (1.0 / mixed[DH : DH + 1])).astype(jnp.bfloat16).T
        at = spot(local - begin)
        for dx in range(COLS):
            for j in range(2):
                r = (dx * 2 + j) * BLOCK
                outs[dx][j, at, :] = result[r : r + BLOCK]
        number = (2 * chip + (core + half) % 2) * TILES + local
        known = jnp.where(block_row <= number, logits[stream][...], -jnp.inf)
        raised = jnp.exp2((known - jnp.max(known, axis=0, keepdims=True)) * EXP2_SCALE)
        prob = raised * (1.0 / jnp.sum(raised, axis=0, keepdims=True))
        folded = prob[:, :128] + prob[:, 128:256] + prob[:, 256:384] + prob[:, 384:]
        factor = jnp.asarray(number + 1).astype(jnp.float32) * (1.0 / (BLOCK * HPG))
        pooled[pl.ds(local - begin, 1), :] = jnp.sum(folded.T, axis=0, keepdims=True) * factor

    def pair(this, stream, that, other):
        top = jnp.max(tops[stream][...], axis=0, keepdims=True)
        mixed, peak = None, None
        for i in range(STEPS):
            if that is not None:
                near = score(that, other, i)
                peak = near if peak is None else jnp.maximum(peak, near)
            got = weigh(this, stream, i, top)
            mixed = got if mixed is None else mixed + got
        if that is not None:
            tops[other][...] = peak
        finish(this, stream, mixed)

    def step(i, carry):
        even = begin + 2 * i
        pair(even, 0, even + 1, 1)
        turn(even + 2, 0)
        pair(even + 1, 1, even + 2, 0)
        turn(even + 3, 1)
        return carry

    last = begin + count - 2
    turn(begin, 0)
    turn(begin + 1, 1)
    for copy in copies:
        copy.wait()
    padded = [pool[pl.ds(s * PIECE + 2 * TOK, COMP_PAD), :] for s in range(SHARDS)]
    comp[...] = dot(take, jnp.concatenate(padded, axis=0)).astype(jnp.bfloat16)
    peak = score(begin, 0, 0)
    for i in range(1, STEPS):
        peak = jnp.maximum(peak, score(begin, 0, i))
    tops[0][...] = peak
    if count > 2:
        lax.fori_loop(0, count // 2 - 1, step, 0)
    pair(last, 0, last + 1, 1)
    pair(last + 1, 1, None, 0)


SMEM = pl.BlockSpec(memory_space=pltpu.SMEM)
VMEM = pl.BlockSpec(memory_space=pltpu.VMEM)
ANY = pl.BlockSpec(memory_space=pl.ANY)


def grant(mib):
    return pltpu.CompilerParams(vmem_limit_bytes=mib * 2**20)


def bf16(*shape):
    return jax.ShapeDtypeStruct(shape, jnp.bfloat16)


def call_split_pools(place, keys, values, comp):
    return pl.pallas_call(
        split_pools,
        in_specs=[SMEM, VMEM, VMEM, VMEM],
        out_specs=[VMEM, VMEM],
        out_shape=[bf16(PIECE, DH)] * 2,
        name="split_pools",
    )(place, keys, values, comp)


def call_split_queries(place, queries):
    steps = 4
    tokens = TOK // steps
    return pl.pallas_call(
        functools.partial(split_queries, tokens),
        grid=(steps,),
        in_specs=[SMEM, pl.BlockSpec((tokens * 16, DH), lambda i: (i, 0))],
        out_specs=[pl.BlockSpec((2, tokens, DH), lambda i: (0, i, 0))] * PARTS,
        out_shape=[bf16(2, TOK, DH)] * PARTS,
        name="split_queries",
    )(place, queries)


def call_attend(half, begin, count, place, picks, owns, pieces, queries):
    return pl.pallas_call(
        functools.partial(attend, half, begin, count),
        in_specs=[SMEM] * 3 + [ANY] * (2 * CHIPS) + [VMEM] * COLS,
        out_specs=[VMEM] * (COLS + 1),
        out_shape=[bf16(2, count * BLOCK, DH)] * COLS + [jax.ShapeDtypeStruct((count, NBLK), jnp.float32)],
        scratch_shapes=[
            pltpu.VMEM((SHARDS * PIECE, DH), jnp.bfloat16),
            pltpu.VMEM((NBLK, DH), jnp.bfloat16),
            pltpu.VMEM((2 * BLOCK, DH), jnp.bfloat16),
        ]
        + [pltpu.VMEM((2 * DH, ROWS), jnp.bfloat16)] * 2
        + [pltpu.VMEM((KEYS, ROWS), jnp.float32)] * 2
        + [pltpu.VMEM((NBLK, ROWS), jnp.float32)] * 2
        + [pltpu.VMEM((8, ROWS), jnp.float32)] * 2
        + [pltpu.SemaphoreType.DMA((2 * CHIPS,))],
        compiler_params=grant(28),
        name="attend",
    )(place, picks, owns, *pieces, *[queries[2 * dx + half] for dx in range(COLS)])


def call_join_outputs(place, parts):
    return pl.pallas_call(
        join_outputs,
        in_specs=[SMEM] + [VMEM] * len(parts),
        out_specs=ANY,
        out_shape=bf16(TOK * 16, DH),
        scratch_shapes=[pltpu.VMEM((TOK * 16, DH), jnp.bfloat16), pltpu.SemaphoreType.DMA((TOK // 128,))],
        compiler_params=grant(16),
        name="join_outputs",
    )(place, *parts)


def by_seq(value, move):
    return lax.ppermute(value, "seq", [(s, move(s // 2, s % 2)) for s in range(SHARDS)])


def to_seq(chip, core):
    return chip % CHIPS * 2 + core % 2


def by_part(value, dx, dc, back):
    if dx == 0 and dc == 0:
        return value
    pairs = []
    for s in range(SHARDS):
        for x in range(COLS):
            there = (s ^ dc) * COLS + (x + dx) % COLS
            here = s * COLS + x
            pairs.append((there, here) if back else (here, there))
    return lax.ppermute(value, ("seq", "head"), pairs)


def whole(queries, key_rows, value_rows, compressed, chosen):
    seq = lax.axis_index("seq")
    col = lax.axis_index("head")
    chip, core = seq // 2, seq % 2
    place = jnp.stack([col, core, chip]).astype(jnp.int32)
    own, other = call_split_pools(
        place, key_rows.reshape(TOK * GROUPS, DH), value_rows.reshape(TOK * GROUPS, DH), compressed.reshape(TILES * GROUPS, DH)
    )
    pieces = [None] * (2 * CHIPS)
    pieces[0] = own
    pieces[1] = by_seq(other, lambda z, c: to_seq(z, c + 1))
    up, down = [own, other], [own, other]
    for k in range(1, 4):
        for h in range(2):
            turn = h if k == 1 else 0
            up[h] = by_seq(up[h], lambda z, c: to_seq(z + 1, c + turn))
            down[h] = by_seq(down[h], lambda z, c: to_seq(z - 1, c + turn))
            pieces[2 * (CHIPS - k) + h] = up[h]
            pieces[2 * k + h] = down[h]
    pieces[2 * 4] = by_seq(up[0], lambda z, c: to_seq(z + 1, c))
    pieces[2 * 4 + 1] = by_seq(down[1], lambda z, c: to_seq(z - 1, c))
    parts = call_split_queries(place, queries.reshape(TOK * 16, DH))
    moved = []
    for k in range(PARTS):
        moved.append(by_part(parts[k], k // 2, k % 2, False))
    groups = chosen[0].transpose(1, 0, 2)
    mine = lax.dynamic_index_in_dim(groups, 2 * col + core, 0, False)
    theirs = lax.dynamic_index_in_dim(groups, 2 * col + 1 - core, 0, False)
    theirs = by_seq(theirs, lambda z, c: to_seq(z, c + 1))
    blocks = jnp.stack([mine, theirs])
    shard = 2 * chip + (core + jnp.arange(2, dtype=jnp.int32)) % 2
    number = shard[:, None] * TILES + jnp.arange(TILES, dtype=jnp.int32)
    picks = (blocks // TILES * PIECE + blocks % TILES * BLOCK).reshape(-1)
    owns = jnp.where(blocks == number[..., None], BLOCK, 0).reshape(-1)
    joined, sums = [], []
    for half, begin, count in CHUNKS:
        *outs, rows = call_attend(half, begin, count, place, picks, owns, pieces, moved)
        back = [None] * COLS
        for dx in (2, 1, 3, 0):
            back[dx] = by_part(outs[dx], dx, half, True)
        joined += back
        sums.append(rows)
    came = by_seq(sums[0], lambda z, c: to_seq(z, c + 1))
    attended = call_join_outputs(place, joined)
    keep = jnp.concatenate(sums[1:])
    both = jnp.where(core == 0, jnp.stack([keep, came], axis=1), jnp.stack([came, keep], axis=1))
    return both[None], attended.reshape(1, TOK, 2, GROUPS, DH)


def solution(mesh):
    placed = (
        P("batch", "seq", "head", None, None),
        P("batch", "seq", None, None),
        P("batch", "seq", None, None),
        P("batch", "seq", None, None),
        P("batch", "seq", None, None),
    )
    return jax.shard_map(
        whole,
        mesh=mesh,
        in_specs=placed,
        out_specs=(P("batch", "seq", "head", None), P("batch", "seq", "head", None, None)),
        check_vma=False,
    )
```

```python
import functools
import math

import jax
import jax.numpy as jnp
from jax import lax
from jax.experimental import pallas as pl
from jax.experimental.pallas import tpu as pltpu
from jax.sharding import PartitionSpec as P


HPG = 8
GROUPS = 8
DH = 128
BLOCK = 64
TOPN = 16
NBLK = 128
SHARDS = 16
CHIPS = 8
COLS = 4
TOK = 512
TILES = 8
COMP_PAD = 16
PIECE = 2 * TOK + COMP_PAD
PARTS = 8
CHUNKS = ((1, 0, 8), (0, 0, 6), (0, 6, 2))
EARLY = tuple((k, h) for k in (0, 1, 2, 3, 5, 6, 7) for h in range(2))
LATE = ((4, 0), (4, 1))
KEYS = TOPN * BLOCK
ROWS = HPG * BLOCK
COMP_ROWS = SHARDS * COMP_PAD
STEPS = 4
STEP_BLOCKS = TOPN // STEPS
STEP_KEYS = KEYS // STEPS
STEP_COMP = NBLK // STEPS
ONES = 16
FAR = -1.0e9
EXP2_SCALE = DH**-0.5 * math.log2(math.e)


def iota(shape, dim):
    return lax.broadcasted_iota(jnp.int32, shape, dim)


def dot(lhs, rhs, dims=(((1,), (0,)), ((), ()))):
    return lax.dot_general(lhs, rhs, dims, preferred_element_type=jnp.float32)


def one_hot(cond):
    return jnp.where(cond, 1.0, 0.0).astype(jnp.bfloat16)


def split_pools(place, keys, values, comp, own, other):
    mine = place[0] * 2 + place[1]
    theirs = place[0] * 2 + 1 - place[1]
    step = 32
    row = iota((2 * step, step * GROUPS), 0)
    col = iota((2 * step, step * GROUPS), 1)
    group = jnp.where(row < step, mine, theirs)
    pick = one_hot(col == (row % step) * GROUPS + group)
    for i in range(TOK // step):
        rows = pl.ds(i * step * GROUPS, step * GROUPS)
        both = jnp.concatenate([keys[rows, :], values[rows, :]], axis=1)
        got = dot(pick, both).astype(jnp.bfloat16)
        own[pl.ds(i * step, step), :] = got[:step, :DH]
        own[pl.ds(TOK + i * step, step), :] = got[:step, DH:]
        other[pl.ds(i * step, step), :] = got[step:, :DH]
        other[pl.ds(TOK + i * step, step), :] = got[step:, DH:]
    row = iota((2 * COMP_PAD, TILES * GROUPS), 0)
    col = iota((2 * COMP_PAD, TILES * GROUPS), 1)
    group = jnp.where(row < COMP_PAD, mine, theirs)
    block = row % COMP_PAD
    got = dot(one_hot((col == block * GROUPS + group) & (block < TILES)), comp[...]).astype(jnp.bfloat16)
    own[pl.ds(2 * TOK, COMP_PAD), :] = got[:COMP_PAD]
    other[pl.ds(2 * TOK, COMP_PAD), :] = got[COMP_PAD:]


def row_of(r, place):
    part = r // 32
    head = (r // 16) % 2
    token = r % 16
    group = 2 * ((place[0] + part // 2) % COLS) + (place[1] + part % 2) % 2
    return token * 16 + head * GROUPS + group


def split_queries(tokens, place, queries, *parts):
    shape = (256, 256)
    pick = one_hot(iota(shape, 1) == row_of(iota(shape, 0), place))
    for i in range(tokens // 32):
        pair = jnp.concatenate([queries[pl.ds(i * 512, 256), :], queries[pl.ds(i * 512 + 256, 256), :]], axis=1)
        got = dot(pick, pair).astype(jnp.bfloat16)
        for k in range(PARTS):
            for j in range(2):
                rows = got[k * 32 + j * 16 : k * 32 + j * 16 + 16]
                parts[k][j, pl.ds(i * 32, 16), :] = rows[:, :DH]
                parts[k][j, pl.ds(i * 32 + 16, 16), :] = rows[:, DH:]


def join_outputs(place, *refs):
    *parts, out, result, sems = refs
    chunks = [parts[c * COLS : (c + 1) * COLS] for c in range(len(CHUNKS))]

    def some(k, j, token):
        for (half, begin, count), group in zip(CHUNKS, chunks):
            at = token - begin * BLOCK
            if half == k % 2 and 0 <= at < count * BLOCK:
                return group[k // 2][j, pl.ds(at, 16), :]

    shape = (256, 256)
    pick = one_hot(iota(shape, 0) == row_of(iota(shape, 1), place))
    copies = []
    for i in range(TOK // 32):
        halves = []
        for h in range(2):
            token = i * 32 + h * 16
            halves.append(jnp.concatenate([some(k, j, token) for k in range(PARTS) for j in range(2)], axis=0))
        got = dot(pick, jnp.concatenate(halves, axis=1)).astype(jnp.bfloat16)
        result[pl.ds(i * 512, 256), :] = got[:, :DH]
        result[pl.ds(i * 512 + 256, 256), :] = got[:, DH:]
        if i % 4 == 3:
            rows = pl.ds((i - 3) * 512, 2048)
            copies.append(pltpu.make_async_copy(result.at[rows, :], out.at[rows, :], sems.at[i // 4]))
            copies[-1].start()
    for copy in copies:
        copy.wait()


def copies_of(place, pieces, names, pool, sems):
    copies = []
    for i, (k, h) in enumerate(names):
        slot = 2 * ((place[2] + k) % CHIPS) + (place[1] + h) % 2
        rows = pl.ds(pl.multiple_of(slot * PIECE, COMP_PAD), PIECE)
        copies.append(pltpu.make_async_copy(pieces[i], pool.at[rows, :], sems.at[i]))
    for copy in copies:
        copy.start()
    return copies


def stage(place, *refs):
    *pieces, pool, sems = refs
    for copy in copies_of(place, pieces, EARLY, pool, sems):
        copy.wait()


def attend(half, begin, count, fresh, place, picks, owns, given, *refs):
    pieces, refs = (refs[: len(LATE)], refs[len(LATE) :]) if fresh else ((), refs)
    queries, refs = refs[:COLS], refs[COLS:]
    outs, refs = refs[:COLS], refs[COLS:]
    pooled, *refs = refs
    pool, refs = (refs[0], refs[1:]) if fresh else (given, refs)
    comp, mask, *rest, sems = refs
    turned, scores, logits, tops = rest[0:2], rest[2:4], rest[4:6], rest[6:8]
    core, chip = place[1], place[2]
    copies = copies_of(place, pieces, LATE, pool, sems) if fresh else []
    shape = (2 * BLOCK, DH)
    row = iota(shape, 0)
    hidden = (row >= BLOCK) & (row - BLOCK > iota(shape, 1))
    mask[...] = jnp.where(hidden, FAR, 0.0).astype(jnp.bfloat16)
    shape = (DH, ROWS)
    for stream in range(2):
        turned[stream][pl.ds(DH, DH), :] = one_hot(iota(shape, 0) == iota(shape, 1) % BLOCK)
    shape = (NBLK, COMP_ROWS)
    take = one_hot(iota(shape, 1) == iota(shape, 0) // TILES * COMP_PAD + iota(shape, 0) % TILES)
    block_row = iota((NBLK, ROWS), 0)
    ones = jnp.full((ONES, STEP_KEYS), 1.0, jnp.bfloat16)

    def spot(local):
        return pl.ds(local * BLOCK if isinstance(local, int) else pl.multiple_of(local * BLOCK, BLOCK), BLOCK)

    def block_of(local, b, offset):
        start = picks[(half * TILES + local) * TOPN + b] + offset
        return pool[pl.ds(pl.multiple_of(start, COMP_PAD), BLOCK), :]

    def mask_of(local, b):
        start = owns[(half * TILES + local) * TOPN + b]
        return mask[pl.ds(pl.multiple_of(start, BLOCK), BLOCK), :]

    def turn(local, stream):
        at = spot(local)
        query = jnp.concatenate([queries[dx][j, at, :] for dx in range(COLS) for j in range(2)], axis=0)
        turned[stream][pl.ds(0, DH), :] = query.T

    def score(local, stream, i):
        keys = []
        for b in range(i * STEP_BLOCKS, (i + 1) * STEP_BLOCKS):
            keys.append(jnp.concatenate([block_of(local, b, 0), mask_of(local, b)], axis=1))
        some = comp[pl.ds(i * STEP_COMP, STEP_COMP), :]
        keys.append(jnp.concatenate([some, jnp.zeros_like(some)], axis=1))
        got = dot(jnp.concatenate(keys, axis=0), turned[stream][...])
        near = got[:STEP_KEYS]
        scores[stream][pl.ds(i * STEP_KEYS, STEP_KEYS), :] = near
        logits[stream][pl.ds(i * STEP_COMP, STEP_COMP), :] = got[STEP_KEYS:]
        return jnp.max(near.reshape(STEP_KEYS // 8, 8, ROWS), axis=0)

    def weigh(local, stream, i, top):
        weight = jnp.exp2((scores[stream][pl.ds(i * STEP_KEYS, STEP_KEYS), :] - top) * EXP2_SCALE).astype(jnp.bfloat16)
        blocks = [block_of(local, b, TOK) for b in range(i * STEP_BLOCKS, (i + 1) * STEP_BLOCKS)]
        values = jnp.concatenate([jnp.concatenate(blocks, axis=0).T, ones], axis=0)
        return dot(values, weight)

    def finish(local, stream, mixed):
        result = (mixed[:DH] * (1.0 / mixed[DH : DH + 1])).astype(jnp.bfloat16).T
        at = spot(local - begin)
        for dx in range(COLS):
            for j in range(2):
                r = (dx * 2 + j) * BLOCK
                outs[dx][j, at, :] = result[r : r + BLOCK]
        number = (2 * chip + (core + half) % 2) * TILES + local
        known = jnp.where(block_row <= number, logits[stream][...], -jnp.inf)
        raised = jnp.exp2((known - jnp.max(known, axis=0, keepdims=True)) * EXP2_SCALE)
        prob = raised * (1.0 / jnp.sum(raised, axis=0, keepdims=True))
        folded = prob[:, :128] + prob[:, 128:256] + prob[:, 256:384] + prob[:, 384:]
        factor = jnp.asarray(number + 1).astype(jnp.float32) * (1.0 / (BLOCK * HPG))
        pooled[pl.ds(local - begin, 1), :] = jnp.sum(folded.T, axis=0, keepdims=True) * factor

    def pair(this, stream, that, other):
        top = jnp.max(tops[stream][...], axis=0, keepdims=True)
        mixed, peak = None, None
        for i in range(STEPS):
            if that is not None:
                near = score(that, other, i)
                peak = near if peak is None else jnp.maximum(peak, near)
            got = weigh(this, stream, i, top)
            mixed = got if mixed is None else mixed + got
        if that is not None:
            tops[other][...] = peak
        finish(this, stream, mixed)

    def step(i, carry):
        even = begin + 2 * i
        pair(even, 0, even + 1, 1)
        turn(even + 2, 0)
        pair(even + 1, 1, even + 2, 0)
        turn(even + 3, 1)
        return carry

    last = begin + count - 2
    turn(begin, 0)
    turn(begin + 1, 1)
    for copy in copies:
        copy.wait()
    padded = [pool[pl.ds(s * PIECE + 2 * TOK, COMP_PAD), :] for s in range(SHARDS)]
    comp[...] = dot(take, jnp.concatenate(padded, axis=0)).astype(jnp.bfloat16)
    peak = score(begin, 0, 0)
    for i in range(1, STEPS):
        peak = jnp.maximum(peak, score(begin, 0, i))
    tops[0][...] = peak
    if count > 2:
        lax.fori_loop(0, count // 2 - 1, step, 0)
    pair(last, 0, last + 1, 1)
    pair(last + 1, 1, None, 0)


SMEM = pl.BlockSpec(memory_space=pltpu.SMEM)
VMEM = pl.BlockSpec(memory_space=pltpu.VMEM)
ANY = pl.BlockSpec(memory_space=pl.ANY)


def grant(mib):
    return pltpu.CompilerParams(vmem_limit_bytes=mib * 2**20)


def bf16(*shape):
    return jax.ShapeDtypeStruct(shape, jnp.bfloat16)


def call_split_pools(place, keys, values, comp):
    return pl.pallas_call(
        split_pools,
        in_specs=[SMEM, VMEM, VMEM, VMEM],
        out_specs=[VMEM, VMEM],
        out_shape=[bf16(PIECE, DH)] * 2,
        name="split_pools",
    )(place, keys, values, comp)


def call_split_queries(place, queries):
    steps = 4
    tokens = TOK // steps
    return pl.pallas_call(
        functools.partial(split_queries, tokens),
        grid=(steps,),
        in_specs=[SMEM, pl.BlockSpec((tokens * 16, DH), lambda i: (i, 0))],
        out_specs=[pl.BlockSpec((2, tokens, DH), lambda i: (0, i, 0))] * PARTS,
        out_shape=[bf16(2, TOK, DH)] * PARTS,
        name="split_queries",
    )(place, queries)


def call_stage(place, pieces):
    return pl.pallas_call(
        stage,
        in_specs=[SMEM] + [ANY] * len(EARLY),
        out_specs=VMEM,
        out_shape=bf16(SHARDS * PIECE, DH),
        scratch_shapes=[pltpu.SemaphoreType.DMA((len(EARLY),))],
        compiler_params=grant(12),
        name="stage",
    )(place, *[pieces[2 * k + h] for k, h in EARLY])


def call_attend(chunk, place, picks, owns, pool, late, queries):
    half, begin, count = chunk
    fresh = bool(late)
    return pl.pallas_call(
        functools.partial(attend, half, begin, count, fresh),
        in_specs=[SMEM] * 3 + [VMEM] + [ANY] * len(late) + [VMEM] * COLS,
        out_specs=[VMEM] * (COLS + 1 + fresh),
        out_shape=[bf16(2, count * BLOCK, DH)] * COLS
        + [jax.ShapeDtypeStruct((count, NBLK), jnp.float32)]
        + [bf16(SHARDS * PIECE, DH)] * fresh,
        input_output_aliases={3: COLS + 1} if fresh else {},
        scratch_shapes=[
            pltpu.VMEM((NBLK, DH), jnp.bfloat16),
            pltpu.VMEM((2 * BLOCK, DH), jnp.bfloat16),
        ]
        + [pltpu.VMEM((2 * DH, ROWS), jnp.bfloat16)] * 2
        + [pltpu.VMEM((KEYS, ROWS), jnp.float32)] * 2
        + [pltpu.VMEM((NBLK, ROWS), jnp.float32)] * 2
        + [pltpu.VMEM((8, ROWS), jnp.float32)] * 2
        + [pltpu.SemaphoreType.DMA((len(LATE),))],
        compiler_params=grant(28),
        name="attend",
    )(place, picks, owns, pool, *late, *[queries[2 * dx + half] for dx in range(COLS)])


def call_join_outputs(place, parts):
    return pl.pallas_call(
        join_outputs,
        in_specs=[SMEM] + [VMEM] * len(parts),
        out_specs=ANY,
        out_shape=bf16(TOK * 16, DH),
        scratch_shapes=[pltpu.VMEM((TOK * 16, DH), jnp.bfloat16), pltpu.SemaphoreType.DMA((TOK // 128,))],
        compiler_params=grant(16),
        name="join_outputs",
    )(place, *parts)


def by_seq(value, move):
    return lax.ppermute(value, "seq", [(s, move(s // 2, s % 2)) for s in range(SHARDS)])


def to_seq(chip, core):
    return chip % CHIPS * 2 + core % 2


def by_part(value, dx, dc, back):
    if dx == 0 and dc == 0:
        return value
    pairs = []
    for s in range(SHARDS):
        for x in range(COLS):
            there = (s ^ dc) * COLS + (x + dx) % COLS
            here = s * COLS + x
            pairs.append((there, here) if back else (here, there))
    return lax.ppermute(value, ("seq", "head"), pairs)


def whole(queries, key_rows, value_rows, compressed, chosen):
    seq = lax.axis_index("seq")
    col = lax.axis_index("head")
    chip, core = seq // 2, seq % 2
    place = jnp.stack([col, core, chip]).astype(jnp.int32)
    own, other = call_split_pools(
        place, key_rows.reshape(TOK * GROUPS, DH), value_rows.reshape(TOK * GROUPS, DH), compressed.reshape(TILES * GROUPS, DH)
    )
    pieces = [None] * (2 * CHIPS)
    pieces[0] = own
    pieces[1] = by_seq(other, lambda z, c: to_seq(z, c + 1))
    up, down = [own, other], [own, other]
    for k in range(1, 4):
        for h in range(2):
            turn = h if k == 1 else 0
            up[h] = by_seq(up[h], lambda z, c: to_seq(z + 1, c + turn))
            down[h] = by_seq(down[h], lambda z, c: to_seq(z - 1, c + turn))
            pieces[2 * (CHIPS - k) + h] = up[h]
            pieces[2 * k + h] = down[h]
    pieces[2 * 4] = by_seq(up[0], lambda z, c: to_seq(z + 1, c))
    pieces[2 * 4 + 1] = by_seq(down[1], lambda z, c: to_seq(z - 1, c))
    parts = call_split_queries(place, queries.reshape(TOK * 16, DH))
    moved = []
    for k in range(PARTS):
        moved.append(by_part(parts[k], k // 2, k % 2, False))
    groups = chosen[0].transpose(1, 0, 2)
    mine = lax.dynamic_index_in_dim(groups, 2 * col + core, 0, False)
    theirs = lax.dynamic_index_in_dim(groups, 2 * col + 1 - core, 0, False)
    theirs = by_seq(theirs, lambda z, c: to_seq(z, c + 1))
    blocks = jnp.stack([mine, theirs])
    shard = 2 * chip + (core + jnp.arange(2, dtype=jnp.int32)) % 2
    number = shard[:, None] * TILES + jnp.arange(TILES, dtype=jnp.int32)
    picks = (blocks // TILES * PIECE + blocks % TILES * BLOCK).reshape(-1)
    owns = jnp.where(blocks == number[..., None], BLOCK, 0).reshape(-1)
    pool = call_stage(place, pieces)
    joined, sums = [], []
    late = [pieces[2 * k + h] for k, h in LATE]
    for chunk in CHUNKS:
        half = chunk[0]
        *outs, rows = call_attend(chunk, place, picks, owns, pool, late, moved)
        if late:
            late, rows, pool = [], outs.pop(), rows
        back = [None] * COLS
        for dx in (2, 1, 3, 0):
            back[dx] = by_part(outs[dx], dx, half, True)
        joined += back
        sums.append(rows)
    came = by_seq(sums[0], lambda z, c: to_seq(z, c + 1))
    attended = call_join_outputs(place, joined)
    keep = jnp.concatenate(sums[1:])
    both = jnp.where(core == 0, jnp.stack([keep, came], axis=1), jnp.stack([came, keep], axis=1))
    return both[None], attended.reshape(1, TOK, 2, GROUPS, DH)


def solution(mesh):
    placed = (
        P("batch", "seq", "head", None, None),
        P("batch", "seq", None, None),
        P("batch", "seq", None, None),
        P("batch", "seq", None, None),
        P("batch", "seq", None, None),
    )
    return jax.shard_map(
        whole,
        mesh=mesh,
        in_specs=placed,
        out_specs=(P("batch", "seq", "head", None), P("batch", "seq", "head", None, None)),
        check_vma=False,
    )
```
